16 devices in a mesh: dp: 2 (over z), tp: 8 (over y, x, core).
Axes of the slice: x: 2, y: 2, z: 2, core: 2. Of those that a mesh axis runs over, the one named last changes fastest.
Arguments:
- x_in: bfloat16 [8192, 4096], P(('dp', 'tp')), parts along dimension 0
- grad_out: bfloat16 [8192, 4096], P(('dp', 'tp')), parts along dimension 0
- positions: int32 [8192], P('dp'), parts along dimension 0
- norm_gain: float32 [4096], replicated
- w_query: bfloat16 [4096, 4096], P(None, 'tp')
- w_key: bfloat16 [4096, 1024], replicated
- w_value: bfloat16 [4096, 1024], replicated
- w_out: bfloat16 [4096, 4096], P('tp')
Outputs:
- output 1: bfloat16 [8192, 4096], P(('dp', 'tp')), parts along dimension 0
- output 2: bfloat16 [8192, 4096], P(('dp', 'tp')), parts along dimension 0
- output 3: bfloat16 [8192, 4096], P('dp', 'tp'), parts along dimension 0
- output 4: float32 [8192, 1024], P('dp', 'tp'), parts along dimension 0
- output 5: float32 [8192, 1024], P('dp', 'tp'), parts along dimension 0
- output 6: bfloat16 [8192, 4096], P(('dp', 'tp')), parts along dimension 0
- output 7: float32 [8192], P('dp'), parts along dimension 0
There are 2 independent parts. The reference program is written for one: setup_inputs(seed, part) draws one part's arguments, and reference() takes and returns one part's arrays. A program takes and returns all parts, laid end to end along the dimension named above; an argument that names none is the same for every part.
All inputs are finite; a program needn't handle non-finite values.
Results may differ from the reference program's by a relative error of at most 0.0183672.
Values are sent between devices in bfloat16 or wider.
A program may use at most 1 GiB of HBM per device.

```python
import functools
import jax
import jax.numpy as jnp
from jax import lax

D_MODEL = 4096
Q_HEADS = 32
KV_HEADS = 8
HEAD_DIM = 128
TP_SIZE = 8
SEQ_LEN = 4096
QUERY_BLOCK = 128
NUM_DOCS = 4
KV_REPEAT = TP_SIZE // KV_HEADS
GROUP_SIZE = Q_HEADS // KV_HEADS
SCORE_SCALE = HEAD_DIM ** -0.5
ROPE_THETA = 1000000.0
NORM_EPS = 1e-05


def draw_positions(pos_key):
    starts = jax.random.randint(pos_key, (NUM_DOCS - 1,), 1, SEQ_LEN)
    tok_idx = jnp.arange(SEQ_LEN, dtype=jnp.int32)
    doc_start = jnp.max(jnp.where(starts[None, :] <= tok_idx[:, None], starts[None, :], 0), axis=1)
    return (tok_idx - doc_start).astype(jnp.int32)


def setup_inputs(seed: int = 0, part: int = 0) -> dict:
    root_key = jax.random.key(seed)
    shared_key, part_root = jax.random.split(root_key)
    part_key = jax.random.fold_in(part_root, part)
    key_x, key_dy, key_pos = jax.random.split(part_key, 3)
    key_g, key_q, key_k, key_v, key_o = jax.random.split(shared_key, 5)
    q_width = Q_HEADS * HEAD_DIM
    kv_width = KV_HEADS * HEAD_DIM
    in_scale = D_MODEL ** -0.5
    x_in = 0.25 * jax.random.normal(key_x, (SEQ_LEN, D_MODEL), jnp.float32)
    grad_out = jax.random.normal(key_dy, (SEQ_LEN, D_MODEL), jnp.float32)
    positions = draw_positions(key_pos)
    norm_gain = jax.random.uniform(key_g, (D_MODEL,), jnp.float32, 0.5, 1.5)
    w_query = jax.random.normal(key_q, (D_MODEL, q_width), jnp.float32) * in_scale
    w_key = jax.random.normal(key_k, (D_MODEL, kv_width), jnp.float32) * in_scale
    w_value = jax.random.normal(key_v, (D_MODEL, kv_width), jnp.float32) * in_scale
    w_out = jax.random.normal(key_o, (q_width, D_MODEL), jnp.float32) * (2.0 * q_width ** -0.5)
    return {'x_in': x_in.astype(jnp.bfloat16), 'grad_out': grad_out.astype(jnp.bfloat16), 'positions': positions, 'norm_gain': norm_gain, 'w_query': w_query.astype(jnp.bfloat16), 'w_key': w_key.astype(jnp.bfloat16), 'w_value': w_value.astype(jnp.bfloat16), 'w_out': w_out.astype(jnp.bfloat16)}


def apply_rope(tensor, cos_t, sin_t):
    half_dim = HEAD_DIM // 2
    t_f32 = tensor.astype(jnp.float32)
    lead_half = t_f32[..., :half_dim]
    tail_half = t_f32[..., half_dim:]
    return jnp.concatenate([lead_half * cos_t - tail_half * sin_t, tail_half * cos_t + lead_half * sin_t], axis=-1).astype(jnp.bfloat16)


def forward_one(x_f32, norm_gain, w_query, w_key_f32, w_value_f32, w_out, positions):
    inv_rms = lax.rsqrt(jnp.mean(x_f32 * x_f32, axis=-1, keepdims=True) + NORM_EPS)
    hidden = (x_f32 * inv_rms * norm_gain).astype(jnp.bfloat16)
    hidden_f32 = hidden.astype(jnp.float32)
    query_proj = jnp.dot(hidden, w_query, preferred_element_type=jnp.float32).astype(jnp.bfloat16)
    key_proj = jnp.dot(hidden_f32, w_key_f32, preferred_element_type=jnp.float32).astype(jnp.bfloat16)
    value_proj = jnp.dot(hidden_f32, w_value_f32, preferred_element_type=jnp.float32).astype(jnp.bfloat16)
    exponents = jnp.arange(0, HEAD_DIM, 2, dtype=jnp.float32) / HEAD_DIM
    angles = positions.astype(jnp.float32)[:, None] * jnp.power(ROPE_THETA, -exponents)[None, :]
    cos_t = jnp.cos(angles)
    sin_t = jnp.sin(angles)
    q_rot = apply_rope(query_proj.reshape(SEQ_LEN, KV_HEADS, GROUP_SIZE, HEAD_DIM), cos_t[:, None, None, :], sin_t[:, None, None, :])
    k_rot = apply_rope(key_proj.reshape(SEQ_LEN, KV_HEADS, HEAD_DIM), cos_t[:, None, :], sin_t[:, None, :])
    key_f32 = k_rot.astype(jnp.float32)
    value_f32 = value_proj.reshape(SEQ_LEN, KV_HEADS, HEAD_DIM).astype(jnp.float32)
    col_idx = jnp.arange(SEQ_LEN, dtype=jnp.int32)
    key_doc = positions - col_idx

    def one_block(blk_item):
        q_blk, q_pos, row_idx = blk_item
        scores = jnp.einsum('qkgd,skd->kgqs', q_blk.astype(jnp.float32), key_f32) * SCORE_SCALE
        keep_mask = (col_idx[None, :] <= row_idx[:, None]) & (key_doc[None, :] == (q_pos - row_idx)[:, None])
        scores = jnp.where(keep_mask, scores, -1e30)
        prob_blk = jax.nn.softmax(scores, axis=-1).astype(jnp.bfloat16).astype(jnp.float32)
        return jnp.einsum('kgqs,skd->qkgd', prob_blk, value_f32).astype(jnp.bfloat16)

    num_blk = SEQ_LEN // QUERY_BLOCK
    blk_out = lax.map(jax.checkpoint(one_block), (q_rot.reshape(num_blk, QUERY_BLOCK, KV_HEADS, GROUP_SIZE, HEAD_DIM), positions.reshape(num_blk, QUERY_BLOCK), col_idx.reshape(num_blk, QUERY_BLOCK)))
    attn_flat = blk_out.reshape(SEQ_LEN, Q_HEADS * HEAD_DIM)
    attn_mix = jnp.dot(attn_flat, w_out, preferred_element_type=jnp.float32)
    return (x_f32 + attn_mix).astype(jnp.bfloat16)


def reference(x_in, grad_out, positions, norm_gain, w_query, w_key, w_value, w_out):
    x_f32 = x_in.astype(jnp.float32)
    forward = functools.partial(forward_one, positions=positions)
    result, pull_back = jax.vjp(forward, x_f32, norm_gain, w_query, w_key.astype(jnp.float32), w_value.astype(jnp.float32), w_out)
    d_x, d_gain, d_wq, d_wk, d_wv, d_wo = pull_back(grad_out)
    copy_shape = (D_MODEL, KV_HEADS, KV_REPEAT, HEAD_DIM)
    grad_wk = jnp.broadcast_to(d_wk.reshape(D_MODEL, KV_HEADS, 1, HEAD_DIM), copy_shape).reshape(D_MODEL, TP_SIZE * HEAD_DIM)
    grad_wv = jnp.broadcast_to(d_wv.reshape(D_MODEL, KV_HEADS, 1, HEAD_DIM), copy_shape).reshape(D_MODEL, TP_SIZE * HEAD_DIM)
    return (result, d_x.astype(jnp.bfloat16), d_wq, grad_wk, grad_wv, d_wo, d_gain)
```

```python
import functools
import jax
import jax.numpy as jnp
from jax import lax
from jax.experimental import pallas as pl
from jax.experimental.pallas import tpu as pltpu
from jax.experimental.layout import Layout, with_layout_constraint
from jax.sharding import PartitionSpec as P

HEAD_DIM = 128
SCORE_SCALE = HEAD_DIM ** -0.5
LOG2_SCALE = SCORE_SCALE * 1.4426950408889634
ROPE_THETA = 1000000.0
NORM_EPS = 1e-05
MASKED = -1e30
BQ = 256
BK = 512
VMEM_LIMIT = 60 * 1024 * 1024
NT = (((1,), (1,)), ((), ()))
TN = (((0,), (0,)), ((), ()))
F32 = jnp.float32
BF16 = jnp.bfloat16


def rope_tables(positions):
    exponents = jnp.arange(0, HEAD_DIM, 2, dtype=F32) / HEAD_DIM
    angles = positions.astype(F32)[..., None] * jnp.power(ROPE_THETA, -exponents)
    cos_t, sin_t = jnp.cos(angles), jnp.sin(angles)
    return jnp.concatenate([cos_t, cos_t], axis=-1), jnp.concatenate([-sin_t, sin_t], axis=-1)


def rope(x, cos_t, sin_t):
    x = x.astype(F32)
    return (x * cos_t + pltpu.roll(x, HEAD_DIM // 2, 1) * sin_t).astype(BF16)


def rope_back(x, cos_t, sin_t):
    x = x.astype(F32)
    return (x * cos_t - pltpu.roll(x, HEAD_DIM // 2, 1) * sin_t).astype(BF16)


def stack_heads(x, heads):
    return jnp.concatenate([x[:, h * HEAD_DIM:(h + 1) * HEAD_DIM] for h in range(heads)], axis=0)


def key_loops(i, lo_ref, full_ref, bq, bk, body):
    first = lo_ref[i]
    below = (i * bq) // bk
    last = ((i + 1) * bq + bk - 1) // bk
    mid = jnp.minimum(jnp.maximum(full_ref[i], first), last)
    mid_end = jnp.maximum(mid, jnp.minimum(below, last))
    lax.fori_loop(first, mid, functools.partial(body, True), None)
    lax.fori_loop(mid, mid_end, functools.partial(body, False), None)
    lax.fori_loop(mid_end, last, functools.partial(body, True), None)


def fwd_kernel(heads, lo_ref, full_ref, q_ref, k_ref, v_ref, cos_ref, sin_ref, cosf_ref, sinf_ref, ds_ref, o_ref, lse_ref, k_s, m_s, l_s, acc_s):
    i = pl.program_id(0)
    bq, bk = BQ, BK
    rows = heads * bq

    @pl.when(i == 0)
    def _():
        k_s[...] = rope(k_ref[...], cosf_ref[...], sinf_ref[...])

    cos_t, sin_t = cos_ref[...], sin_ref[...]
    q4 = jnp.concatenate([rope(q_ref[:, h * HEAD_DIM:(h + 1) * HEAD_DIM], cos_t, sin_t) for h in range(heads)], axis=0)
    m_s[...] = jnp.full_like(m_s, MASKED)
    l_s[...] = jnp.zeros_like(l_s)
    acc_s[...] = jnp.zeros_like(acc_s)

    def body(masked, j, _):
        start = pl.multiple_of(j * bk, bk)
        kj = k_s[pl.ds(start, bk), :]
        vj = v_ref[pl.ds(start, bk), :]
        s = lax.dot_general(q4, kj, NT, preferred_element_type=F32) * LOG2_SCALE
        if masked:
            q_idx = i * bq + lax.broadcasted_iota(jnp.int32, (bq, bk), 0)
            k_idx = start + lax.broadcasted_iota(jnp.int32, (bq, bk), 1)
            keep = (k_idx <= q_idx) & (k_idx >= ds_ref[...])
            s = jnp.concatenate([jnp.where(keep, s[h * bq:(h + 1) * bq], MASKED) for h in range(heads)], axis=0)
        m_prev = m_s[...]
        m_new = jnp.maximum(m_prev, jnp.max(s, axis=1, keepdims=True))
        p = jnp.exp2(s - jnp.tile(m_new, (1, bk // HEAD_DIM)))
        alpha = jnp.exp2(m_prev - m_new)
        l_s[...] = l_s[...] * alpha + jnp.sum(p, axis=1, keepdims=True)
        m_s[...] = m_new
        acc_s[...] = acc_s[...] * alpha + jnp.dot(p.astype(BF16), vj, preferred_element_type=F32)

    key_loops(i, lo_ref, full_ref, bq, bk, body)
    l_all = l_s[...]
    o4 = (acc_s[...] / l_all).astype(BF16)
    for h in range(heads):
        o_ref[:, h * HEAD_DIM:(h + 1) * HEAD_DIM] = o4[h * bq:(h + 1) * bq]
    lse = m_s[...] + jnp.log2(l_all)
    lse_ref[0] = lse.T[0:1, :]


def bwd_kernel(heads, n_blk, lo_ref, full_ref, q_ref, k_ref, v_ref, o_ref, do_ref, lse_ref, cos_ref, sin_ref, cosf_ref, sinf_ref, ds_ref, out_ref, k_s, dq_s, dk_s, dv_s):
    i = pl.program_id(0)
    bq, bk = BQ, BK
    rows = heads * bq
    width = heads * HEAD_DIM

    @pl.when(i == 0)
    def _():
        k_s[...] = rope(k_ref[...], cosf_ref[...], sinf_ref[...])
        dk_s[...] = jnp.zeros_like(dk_s)
        dv_s[...] = jnp.zeros_like(dv_s)

    cos_t, sin_t = cos_ref[...], sin_ref[...]
    q4 = jnp.concatenate([rope(q_ref[:, h * HEAD_DIM:(h + 1) * HEAD_DIM], cos_t, sin_t) for h in range(heads)], axis=0)
    do4 = stack_heads(do_ref[...], heads)
    o4 = stack_heads(o_ref[...], heads)
    delta = jnp.sum((do4.astype(F32) * o4.astype(F32)).T, axis=0, keepdims=True)
    lse = lse_ref[0]
    dq_s[...] = jnp.zeros_like(dq_s)

    def body(masked, j, _):
        start = pl.multiple_of(j * bk, bk)
        kj = k_s[pl.ds(start, bk), :]
        vj = v_ref[pl.ds(start, bk), :]
        s = lax.dot_general(kj, q4, NT, preferred_element_type=F32) * LOG2_SCALE
        if masked:
            q_idx = i * bq + lax.broadcasted_iota(jnp.int32, (bk, bq), 1)
            k_idx = start + lax.broadcasted_iota(jnp.int32, (bk, bq), 0)
            keep = (k_idx <= q_idx) & (k_idx >= ds_ref[0])
            s = jnp.concatenate([jnp.where(keep, s[:, h * bq:(h + 1) * bq], MASKED) for h in range(heads)], axis=1)
        p = jnp.exp2(s - lse)
        dp = lax.dot_general(vj, do4, NT, preferred_element_type=F32)
        dv_s[pl.ds(start, bk), :] += jnp.dot(p.astype(BF16), do4, preferred_element_type=F32)
        d_s = (p * (dp - delta)).astype(BF16)
        dk_s[pl.ds(start, bk), :] += jnp.dot(d_s, q4, preferred_element_type=F32)
        dq_s[...] += lax.dot_general(d_s, kj, TN, preferred_element_type=F32)

    key_loops(i, lo_ref, full_ref, bq, bk, body)
    row0 = pl.multiple_of(i * bq, bq)
    for h in range(heads):
        dq = (dq_s[h * bq:(h + 1) * bq, :] * SCORE_SCALE).astype(BF16)
        out_ref[pl.ds(row0, bq), h * HEAD_DIM:(h + 1) * HEAD_DIM] = rope_back(dq, cos_t, sin_t)

    @pl.when(i == n_blk - 1)
    def _():
        dk = (dk_s[...] * SCORE_SCALE).astype(BF16)
        out_ref[:, width:width + HEAD_DIM] = rope_back(dk, cosf_ref[...], sinf_ref[...])
        out_ref[:, width + HEAD_DIM:width + 2 * HEAD_DIM] = dv_s[...].astype(BF16)


def attention_specs(seq, heads):
    width = heads * HEAD_DIM
    q_spec = pl.BlockSpec((BQ, width), lambda i, *_: (i, 0))
    k_spec = pl.BlockSpec((seq, HEAD_DIM), lambda i, *_: (0, heads))
    v_spec = pl.BlockSpec((seq, HEAD_DIM), lambda i, *_: (0, heads + 1))
    tab_spec = pl.BlockSpec((BQ, HEAD_DIM), lambda i, *_: (i, 0))
    tabf_spec = pl.BlockSpec((seq, HEAD_DIM), lambda i, *_: (0, 0))
    row_spec = pl.BlockSpec((1, 1, heads * BQ), lambda i, *_: (i, 0, 0))
    return q_spec, k_spec, v_spec, tab_spec, tabf_spec, row_spec


def attend_forward(lo, full, qkv, cos_t, sin_t, doc_start, heads):
    seq = qkv.shape[0]
    n_blk = seq // BQ
    q_spec, k_spec, v_spec, tab_spec, tabf_spec, row_spec = attention_specs(seq, heads)
    return pl.pallas_call(
        functools.partial(fwd_kernel, heads),
        out_shape=(jax.ShapeDtypeStruct((seq, heads * HEAD_DIM), BF16), jax.ShapeDtypeStruct((n_blk, 1, heads * BQ), F32)),
        grid_spec=pltpu.PrefetchScalarGridSpec(
            num_scalar_prefetch=2, grid=(n_blk,),
            in_specs=[q_spec, k_spec, v_spec, tab_spec, tab_spec, tabf_spec, tabf_spec, pl.BlockSpec((BQ, 1), lambda i, *_: (i, 0))],
            out_specs=[q_spec, row_spec],
            scratch_shapes=[pltpu.VMEM((seq, HEAD_DIM), BF16)] + [pltpu.VMEM((heads * BQ, HEAD_DIM), F32)] * 3),
        compiler_params=pltpu.CompilerParams(dimension_semantics=("arbitrary",), vmem_limit_bytes=VMEM_LIMIT),
        cost_estimate=pl.CostEstimate(flops=4 * heads * seq * seq // 2 * HEAD_DIM, bytes_accessed=16 * 2 ** 20, transcendentals=heads * seq * seq // 2),
        name="attend_fwd",
    )(lo, full, qkv, qkv, qkv, cos_t, sin_t, cos_t, sin_t, doc_start[:, None])


def attend_backward(lo, full, qkv, o, d_o, lse, cos_t, sin_t, doc_start, heads):
    seq = qkv.shape[0]
    n_blk = seq // BQ
    width = heads * HEAD_DIM
    q_spec, k_spec, v_spec, tab_spec, tabf_spec, row_spec = attention_specs(seq, heads)
    return pl.pallas_call(
        functools.partial(bwd_kernel, heads, n_blk),
        out_shape=jax.ShapeDtypeStruct((seq, width + 2 * HEAD_DIM), BF16),
        grid_spec=pltpu.PrefetchScalarGridSpec(
            num_scalar_prefetch=2, grid=(n_blk,),
            in_specs=[q_spec, k_spec, v_spec, q_spec, q_spec, row_spec, tab_spec, tab_spec, tabf_spec, tabf_spec, pl.BlockSpec((1, 1, BQ), lambda i, *_: (i, 0, 0))],
            out_specs=pl.BlockSpec((seq, width + 2 * HEAD_DIM), lambda i, *_: (0, 0)),
            scratch_shapes=[pltpu.VMEM((seq, HEAD_DIM), BF16), pltpu.VMEM((heads * BQ, HEAD_DIM), F32), pltpu.VMEM((seq, HEAD_DIM), F32), pltpu.VMEM((seq, HEAD_DIM), F32)]),
        compiler_params=pltpu.CompilerParams(dimension_semantics=("arbitrary",), vmem_limit_bytes=VMEM_LIMIT),
        cost_estimate=pl.CostEstimate(flops=10 * heads * seq * seq // 2 * HEAD_DIM, bytes_accessed=24 * 2 ** 20, transcendentals=heads * seq * seq // 2),
        name="attend_bwd",
    )(lo, full, qkv, qkv, qkv, o, d_o, lse, cos_t, sin_t, cos_t, sin_t, doc_start.reshape(n_blk, 1, BQ))


def norm_forward(x_f32, norm_gain):
    inv_rms = lax.rsqrt(jnp.mean(x_f32 * x_f32, axis=-1, keepdims=True) + NORM_EPS)
    x_hat = x_f32 * inv_rms
    return (x_hat * norm_gain).astype(BF16), x_hat, inv_rms


def dot32(a, b, dims=(((1,), (0,)), ((), ()))):
    return lax.dot_general(a, b, dims, preferred_element_type=F32)


def row_major(x):
    return with_layout_constraint(x, Layout(major_to_minor=tuple(range(x.ndim))))


def sum_over_tp(value, tp_size):
    step = 1
    while step < tp_size:
        value = value + lax.ppermute(value, 'tp', [(d, d ^ step) for d in range(tp_size)])
        step *= 2
    return value


def solution(mesh):
    tp_size = mesh.shape['tp']
    dp_size = mesh.shape['dp']

    def device_step(x_blk, dy_blk, positions, norm_gain, wq_loc, wk_all, wv_all, wo_loc):
        heads = wq_loc.shape[1] // HEAD_DIM
        width = heads * HEAD_DIM
        rows, d_model = x_blk.shape
        tp_idx, dp_idx = lax.axis_index('tp'), lax.axis_index('dp')
        wk_loc = lax.dynamic_slice_in_dim(wk_all, tp_idx * HEAD_DIM, HEAD_DIM, axis=1)
        wv_loc = lax.dynamic_slice_in_dim(wv_all, tp_idx * HEAD_DIM, HEAD_DIM, axis=1)
        wqkv = jnp.concatenate([wq_loc, wk_loc, wv_loc], axis=1)
        wq_t = wq_loc.T
        share = width // dp_size
        wq_share = lax.dynamic_slice_in_dim(wq_t, dp_idx * share, share, axis=0)
        wo_share = lax.dynamic_slice_in_dim(wo_loc, dp_idx * share, share, axis=0)

        x_f32 = x_blk.astype(F32)
        hidden, x_hat, inv_rms = norm_forward(x_f32, norm_gain)
        h_full = lax.all_gather(hidden, 'tp', axis=0, tiled=True)
        seq = h_full.shape[0]
        dy_in, h_full = lax.optimization_barrier((dy_blk, h_full))
        dy_full = lax.all_gather(dy_in, 'tp', axis=0, tiled=True)

        cos_t, sin_t = rope_tables(positions)
        doc_start = lax.iota(jnp.int32, seq) - positions
        lo = doc_start[::BQ] // BK
        full = (doc_start[BQ - 1::BQ] + BK - 1) // BK

        qkv = dot32(h_full, wqkv).astype(BF16)
        wq_share, qkv = lax.optimization_barrier((wq_share, qkv))
        wq_full_t = lax.all_gather(row_major(wq_share), ('tp', 'dp'), axis=0, tiled=True)
        o, lse = attend_forward(lo, full, qkv, cos_t, sin_t, doc_start, heads)
        o_got = row_major(lax.all_to_all(row_major(o.reshape(tp_size, rows, width)), 'tp', 0, 0))
        dy_full, o_got = lax.optimization_barrier((dy_full, o_got))
        o_rows = row_major(o_got.transpose(1, 0, 2)).reshape(rows, tp_size * width)

        d_o = dot32(dy_full, wo_loc, NT).astype(BF16)
        wo_share, d_o = lax.optimization_barrier((wo_share, d_o))
        wo_full = lax.all_gather(row_major(wo_share), ('tp', 'dp'), axis=0, tiled=True)
        d_qkv = attend_backward(lo, full, qkv, o, d_o, lse, cos_t, sin_t, doc_start, heads)
        got = row_major(lax.all_to_all(row_major(d_qkv.reshape(tp_size, rows, width + 2 * HEAD_DIM)), 'tp', 0, 0))
        got = row_major(got.transpose(1, 0, 2))
        dq_rows = got[:, :, :width].reshape(rows, tp_size * width)
        dk_rows = got[:, :, width:width + HEAD_DIM].reshape(rows, tp_size * HEAD_DIM)
        dv_rows = got[:, :, width + HEAD_DIM:].reshape(rows, tp_size * HEAD_DIM)

        d_wo = dot32(o, dy_full, TN).astype(BF16)
        d_wq = dot32(h_full, d_qkv[:, :width], TN).astype(BF16)
        d_wkv = dot32(h_full, d_qkv[:, width:], TN)
        d_wk, d_wv = d_wkv[:, :HEAD_DIM], d_wkv[:, HEAD_DIM:]

        d_hidden = (dot32(dq_rows, wq_full_t) + (dot32(dk_rows, wk_all, NT) + dot32(dv_rows, wv_all, NT))).astype(BF16)
        d_f32 = d_hidden.astype(F32)
        d_gain = sum_over_tp(jnp.sum(d_f32 * x_hat, axis=0), tp_size)
        scaled = d_f32 * norm_gain
        d_input = inv_rms * (scaled - x_hat * jnp.mean(scaled * x_hat, axis=-1, keepdims=True))
        grad_x = (dy_blk.astype(F32) + d_input).astype(BF16)
        result = (x_f32 + dot32(o_rows, wo_full)).astype(BF16)
        return result, grad_x, d_wq, d_wk, d_wv, d_wo, d_gain

    specs_in = (P(('dp', 'tp'), None), P(('dp', 'tp'), None), P('dp'), P(), P(None, 'tp'), P(), P(), P('tp', None))
    specs_out = (P(('dp', 'tp'), None), P(('dp', 'tp'), None), P('dp', 'tp'), P('dp', 'tp'), P('dp', 'tp'), P(('dp', 'tp'), None), P('dp'))
    return jax.shard_map(device_step, mesh=mesh, in_specs=specs_in, out_specs=specs_out, check_vma=False)
```

```python
import functools
import jax
import jax.numpy as jnp
from jax import lax
from jax.experimental import pallas as pl
from jax.experimental.pallas import tpu as pltpu
from jax.experimental.layout import Layout, with_layout_constraint
from jax.sharding import PartitionSpec as P

HEAD_DIM = 128
SCORE_SCALE = HEAD_DIM ** -0.5
LOG2_SCALE = SCORE_SCALE * 1.4426950408889634
ROPE_THETA = 1000000.0
NORM_EPS = 1e-05
MASKED = -1e30
BQ = 256
BK = 512
VMEM_LIMIT = 60 * 1024 * 1024
NT = (((1,), (1,)), ((), ()))
TN = (((0,), (0,)), ((), ()))
F32 = jnp.float32
BF16 = jnp.bfloat16


def rope_tables(positions):
    exponents = jnp.arange(0, HEAD_DIM, 2, dtype=F32) / HEAD_DIM
    angles = positions.astype(F32)[..., None] * jnp.power(ROPE_THETA, -exponents)
    cos_t, sin_t = jnp.cos(angles), jnp.sin(angles)
    return jnp.concatenate([cos_t, cos_t], axis=-1), jnp.concatenate([-sin_t, sin_t], axis=-1)


def rope(x, cos_t, sin_t):
    x = x.astype(F32)
    return (x * cos_t + pltpu.roll(x, HEAD_DIM // 2, 1) * sin_t).astype(BF16)


def rope_back(x, cos_t, sin_t):
    x = x.astype(F32)
    return (x * cos_t - pltpu.roll(x, HEAD_DIM // 2, 1) * sin_t).astype(BF16)


def stack_heads(x, heads):
    return jnp.concatenate([x[:, h * HEAD_DIM:(h + 1) * HEAD_DIM] for h in range(heads)], axis=0)


def key_loops(i, lo_ref, full_ref, bq, bk, body):
    first = lo_ref[i]
    below = (i * bq) // bk
    last = ((i + 1) * bq + bk - 1) // bk
    mid = jnp.minimum(jnp.maximum(full_ref[i], first), last)
    mid_end = jnp.maximum(mid, jnp.minimum(below, last))
    lax.fori_loop(first, mid, functools.partial(body, True), None)
    lax.fori_loop(mid, mid_end, functools.partial(body, False), None)
    lax.fori_loop(mid_end, last, functools.partial(body, True), None)


def fwd_kernel(heads, lo_ref, full_ref, q_ref, k_ref, v_ref, cos_ref, sin_ref, cosf_ref, sinf_ref, ds_ref, o_ref, lse_ref, k_s, m_s, l_s, acc_s):
    i = pl.program_id(0)
    bq, bk = BQ, BK
    rows = heads * bq

    @pl.when(i == 0)
    def _():
        k_s[...] = rope(k_ref[...], cosf_ref[...], sinf_ref[...])

    cos_t, sin_t = cos_ref[...], sin_ref[...]
    q4 = jnp.concatenate([rope(q_ref[:, h * HEAD_DIM:(h + 1) * HEAD_DIM], cos_t, sin_t) for h in range(heads)], axis=0)
    m_s[...] = jnp.full_like(m_s, MASKED)
    l_s[...] = jnp.zeros_like(l_s)
    acc_s[...] = jnp.zeros_like(acc_s)

    def body(masked, j, _):
        start = pl.multiple_of(j * bk, bk)
        kj = k_s[pl.ds(start, bk), :]
        vj = v_ref[pl.ds(start, bk), :]
        s = lax.dot_general(q4, kj, NT, preferred_element_type=F32) * LOG2_SCALE
        if masked:
            q_idx = i * bq + lax.broadcasted_iota(jnp.int32, (bq, bk), 0)
            k_idx = start + lax.broadcasted_iota(jnp.int32, (bq, bk), 1)
            keep = (k_idx <= q_idx) & (k_idx >= ds_ref[...])
            s = jnp.concatenate([jnp.where(keep, s[h * bq:(h + 1) * bq], MASKED) for h in range(heads)], axis=0)
        m_prev = m_s[...]
        m_new = jnp.maximum(m_prev, jnp.max(s, axis=1, keepdims=True))
        p = jnp.exp2(s - jnp.tile(m_new, (1, bk // HEAD_DIM)))
        alpha = jnp.exp2(m_prev - m_new)
        l_s[...] = l_s[...] * alpha + jnp.sum(p, axis=1, keepdims=True)
        m_s[...] = m_new
        acc_s[...] = acc_s[...] * alpha + jnp.dot(p.astype(BF16), vj, preferred_element_type=F32)

    key_loops(i, lo_ref, full_ref, bq, bk, body)
    l_all = l_s[...]
    o4 = (acc_s[...] / l_all).astype(BF16)
    for h in range(heads):
        o_ref[:, h * HEAD_DIM:(h + 1) * HEAD_DIM] = o4[h * bq:(h + 1) * bq]
    lse = m_s[...] + jnp.log2(l_all)
    lse_ref[0] = lse.T[0:1, :]


def bwd_kernel(heads, n_blk, lo_ref, full_ref, q_ref, k_ref, v_ref, o_ref, do_ref, lse_ref, cos_ref, sin_ref, cosf_ref, sinf_ref, ds_ref, out_ref, k_s, dq_s, dk_s, dv_s):
    i = pl.program_id(0)
    bq, bk = BQ, BK
    rows = heads * bq
    width = heads * HEAD_DIM

    @pl.when(i == 0)
    def _():
        k_s[...] = rope(k_ref[...], cosf_ref[...], sinf_ref[...])
        dk_s[...] = jnp.zeros_like(dk_s)
        dv_s[...] = jnp.zeros_like(dv_s)

    cos_t, sin_t = cos_ref[...], sin_ref[...]
    q4 = jnp.concatenate([rope(q_ref[:, h * HEAD_DIM:(h + 1) * HEAD_DIM], cos_t, sin_t) for h in range(heads)], axis=0)
    do4 = stack_heads(do_ref[...], heads)
    o4 = stack_heads(o_ref[...], heads)
    delta = jnp.sum((do4.astype(F32) * o4.astype(F32)).T, axis=0, keepdims=True)
    lse = lse_ref[0]
    dq_s[...] = jnp.zeros_like(dq_s)

    def body(masked, j, _):
        start = pl.multiple_of(j * bk, bk)
        kj = k_s[pl.ds(start, bk), :]
        vj = v_ref[pl.ds(start, bk), :]
        s = lax.dot_general(kj, q4, NT, preferred_element_type=F32) * LOG2_SCALE
        if masked:
            q_idx = i * bq + lax.broadcasted_iota(jnp.int32, (bk, bq), 1)
            k_idx = start + lax.broadcasted_iota(jnp.int32, (bk, bq), 0)
            keep = (k_idx <= q_idx) & (k_idx >= ds_ref[0])
            s = jnp.concatenate([jnp.where(keep, s[:, h * bq:(h + 1) * bq], MASKED) for h in range(heads)], axis=1)
        p = jnp.exp2(s - lse)
        dp = lax.dot_general(vj, do4, NT, preferred_element_type=F32)
        dv_s[pl.ds(start, bk), :] += jnp.dot(p.astype(BF16), do4, preferred_element_type=F32)
        d_s = (p * (dp - delta)).astype(BF16)
        dk_s[pl.ds(start, bk), :] += jnp.dot(d_s, q4, preferred_element_type=F32)
        dq_s[...] += lax.dot_general(d_s, kj, TN, preferred_element_type=F32)

    key_loops(i, lo_ref, full_ref, bq, bk, body)
    row0 = pl.multiple_of(i * bq, bq)
    for h in range(heads):
        dq = (dq_s[h * bq:(h + 1) * bq, :] * SCORE_SCALE).astype(BF16)
        out_ref[pl.ds(row0, bq), h * HEAD_DIM:(h + 1) * HEAD_DIM] = rope_back(dq, cos_t, sin_t)

    @pl.when(i == n_blk - 1)
    def _():
        dk = (dk_s[...] * SCORE_SCALE).astype(BF16)
        out_ref[:, width:width + HEAD_DIM] = rope_back(dk, cosf_ref[...], sinf_ref[...])
        out_ref[:, width + HEAD_DIM:width + 2 * HEAD_DIM] = dv_s[...].astype(BF16)


def attention_specs(seq, heads):
    width = heads * HEAD_DIM
    q_spec = pl.BlockSpec((BQ, width), lambda i, *_: (i, 0))
    k_spec = pl.BlockSpec((seq, HEAD_DIM), lambda i, *_: (0, heads))
    v_spec = pl.BlockSpec((seq, HEAD_DIM), lambda i, *_: (0, heads + 1))
    tab_spec = pl.BlockSpec((BQ, HEAD_DIM), lambda i, *_: (i, 0))
    tabf_spec = pl.BlockSpec((seq, HEAD_DIM), lambda i, *_: (0, 0))
    row_spec = pl.BlockSpec((1, 1, heads * BQ), lambda i, *_: (i, 0, 0))
    return q_spec, k_spec, v_spec, tab_spec, tabf_spec, row_spec


def attend_forward(lo, full, qkv, cos_t, sin_t, doc_start, heads):
    seq = qkv.shape[0]
    n_blk = seq // BQ
    q_spec, k_spec, v_spec, tab_spec, tabf_spec, row_spec = attention_specs(seq, heads)
    return pl.pallas_call(
        functools.partial(fwd_kernel, heads),
        out_shape=(jax.ShapeDtypeStruct((seq, heads * HEAD_DIM), BF16), jax.ShapeDtypeStruct((n_blk, 1, heads * BQ), F32)),
        grid_spec=pltpu.PrefetchScalarGridSpec(
            num_scalar_prefetch=2, grid=(n_blk,),
            in_specs=[q_spec, k_spec, v_spec, tab_spec, tab_spec, tabf_spec, tabf_spec, pl.BlockSpec((BQ, 1), lambda i, *_: (i, 0))],
            out_specs=[q_spec, row_spec],
            scratch_shapes=[pltpu.VMEM((seq, HEAD_DIM), BF16)] + [pltpu.VMEM((heads * BQ, HEAD_DIM), F32)] * 3),
        compiler_params=pltpu.CompilerParams(dimension_semantics=("arbitrary",), vmem_limit_bytes=VMEM_LIMIT),
        cost_estimate=pl.CostEstimate(flops=4 * heads * seq * seq // 2 * HEAD_DIM, bytes_accessed=16 * 2 ** 20, transcendentals=heads * seq * seq // 2),
        name="attend_fwd",
    )(lo, full, qkv, qkv, qkv, cos_t, sin_t, cos_t, sin_t, doc_start[:, None])


def attend_backward(lo, full, qkv, o, d_o, lse, cos_t, sin_t, doc_start, heads):
    seq = qkv.shape[0]
    n_blk = seq // BQ
    width = heads * HEAD_DIM
    q_spec, k_spec, v_spec, tab_spec, tabf_spec, row_spec = attention_specs(seq, heads)
    return pl.pallas_call(
        functools.partial(bwd_kernel, heads, n_blk),
        out_shape=jax.ShapeDtypeStruct((seq, width + 2 * HEAD_DIM), BF16),
        grid_spec=pltpu.PrefetchScalarGridSpec(
            num_scalar_prefetch=2, grid=(n_blk,),
            in_specs=[q_spec, k_spec, v_spec, q_spec, q_spec, row_spec, tab_spec, tab_spec, tabf_spec, tabf_spec, pl.BlockSpec((1, 1, BQ), lambda i, *_: (i, 0, 0))],
            out_specs=pl.BlockSpec((seq, width + 2 * HEAD_DIM), lambda i, *_: (0, 0)),
            scratch_shapes=[pltpu.VMEM((seq, HEAD_DIM), BF16), pltpu.VMEM((heads * BQ, HEAD_DIM), F32), pltpu.VMEM((seq, HEAD_DIM), F32), pltpu.VMEM((seq, HEAD_DIM), F32)]),
        compiler_params=pltpu.CompilerParams(dimension_semantics=("arbitrary",), vmem_limit_bytes=VMEM_LIMIT),
        cost_estimate=pl.CostEstimate(flops=10 * heads * seq * seq // 2 * HEAD_DIM, bytes_accessed=24 * 2 ** 20, transcendentals=heads * seq * seq // 2),
        name="attend_bwd",
    )(lo, full, qkv, qkv, qkv, o, d_o, lse, cos_t, sin_t, cos_t, sin_t, doc_start.reshape(n_blk, 1, BQ))


def norm_forward(x_f32, norm_gain):
    inv_rms = lax.rsqrt(jnp.mean(x_f32 * x_f32, axis=-1, keepdims=True) + NORM_EPS)
    x_hat = x_f32 * inv_rms
    return (x_hat * norm_gain).astype(BF16), x_hat, inv_rms


def dot32(a, b, dims=(((1,), (0,)), ((), ()))):
    return lax.dot_general(a, b, dims, preferred_element_type=F32)


def row_major(x):
    return with_layout_constraint(x, Layout(major_to_minor=tuple(range(x.ndim))))


def sum_over_tp(value, tp_size):
    step = 1
    while step < tp_size:
        value = value + lax.ppermute(value, 'tp', [(d, d ^ step) for d in range(tp_size)])
        step *= 2
    return value


def grad_mm_kernel(width, owner_ref, *refs):
    g_refs, w_refs, (wk_ref, wv_ref, out_ref, x_s, w_s) = refs[:4], refs[4:8], refs[8:]
    span = width + 2 * HEAD_DIM

    @pl.when(pl.program_id(0) == 0)
    def _():
        for p, g_ref in enumerate(g_refs):
            x_s[:, p * span:(p + 1) * span] = g_ref[0]

    for p, w_ref in enumerate(w_refs):
        head = pl.ds(pl.multiple_of(owner_ref[p] * HEAD_DIM, HEAD_DIM), HEAD_DIM)
        w_s[:, p * span:p * span + width] = w_ref[...]
        w_s[:, p * span + width:p * span + width + HEAD_DIM] = wk_ref[:, head]
        w_s[:, p * span + width + HEAD_DIM:(p + 1) * span] = wv_ref[:, head]
    out_ref[...] = lax.dot_general(x_s[...], w_s[...], NT, preferred_element_type=F32).astype(out_ref.dtype)


def grad_mm(owners, pieces, half, weights, wk_all, wv_all, dtype):
    _, rows, span = pieces[0].shape
    d_model, width = weights[0].shape
    bn = 512
    g_spec = pl.BlockSpec((1, rows, span), lambda j, *_: (half, 0, 0))
    w_spec = pl.BlockSpec((bn, width), lambda j, *_: (j, 0))
    kv_spec = pl.BlockSpec((bn, wk_all.shape[1]), lambda j, *_: (j, 0))
    return pl.pallas_call(
        functools.partial(grad_mm_kernel, width),
        out_shape=jax.ShapeDtypeStruct((rows, d_model), dtype),
        grid_spec=pltpu.PrefetchScalarGridSpec(
            num_scalar_prefetch=1, grid=(d_model // bn,),
            in_specs=[g_spec] * 4 + [w_spec] * 4 + [kv_spec] * 2,
            out_specs=pl.BlockSpec((rows, bn), lambda j, *_: (0, j)),
            scratch_shapes=[pltpu.VMEM((rows, 4 * span), BF16), pltpu.VMEM((bn, 4 * span), BF16)]),
        compiler_params=pltpu.CompilerParams(dimension_semantics=("arbitrary",), vmem_limit_bytes=VMEM_LIMIT),
        cost_estimate=pl.CostEstimate(flops=2 * rows * 4 * span * d_model, bytes_accessed=2 * (4 * span + 2 * rows) * d_model, transcendentals=0),
        name="grad_mm",
    )(owners, *pieces, *weights, wk_all, wv_all)


def mix_mm_kernel(width, *refs):
    o_refs, w_refs, (out_ref, x_s, w_s) = refs[:4], refs[4:8], refs[8:]

    @pl.when(pl.program_id(0) == 0)
    def _():
        for p, o_ref in enumerate(o_refs):
            x_s[:, p * width:(p + 1) * width] = o_ref[0]

    for p, w_ref in enumerate(w_refs):
        w_s[p * width:(p + 1) * width, :] = w_ref[...]
    out_ref[...] = jnp.dot(x_s[...], w_s[...], preferred_element_type=F32).astype(out_ref.dtype)


def mix_mm(pieces, half, weights, dtype):
    _, rows, width = pieces[0].shape
    d_model = weights[0].shape[1]
    bn = 512
    o_spec = pl.BlockSpec((1, rows, width), lambda j: (half, 0, 0))
    w_spec = pl.BlockSpec((width, bn), lambda j: (0, j))
    return pl.pallas_call(
        functools.partial(mix_mm_kernel, width),
        out_shape=jax.ShapeDtypeStruct((rows, d_model), dtype),
        grid=(d_model // bn,),
        in_specs=[o_spec] * 4 + [w_spec] * 4,
        out_specs=pl.BlockSpec((rows, bn), lambda j: (0, j)),
        scratch_shapes=[pltpu.VMEM((rows, 4 * width), BF16), pltpu.VMEM((4 * width, bn), BF16)],
        compiler_params=pltpu.CompilerParams(dimension_semantics=("arbitrary",), vmem_limit_bytes=VMEM_LIMIT),
        cost_estimate=pl.CostEstimate(flops=2 * rows * 4 * width * d_model, bytes_accessed=2 * (4 * width + 2 * rows) * d_model, transcendentals=0),
        name="mix_mm",
    )(*pieces, *weights)


def swap(value, bit, tp_size):
    return lax.ppermute(value, 'tp', [(d, d ^ bit) for d in range(tp_size)])


def group_rows(blocks, me, pair_bit, mate_bit, tp_size):
    def rows_of(owner):
        return jnp.stack([lax.dynamic_index_in_dim(blocks, owner, 0, False), lax.dynamic_index_in_dim(blocks, owner ^ mate_bit, 0, False)])
    pieces = [rows_of(me)]
    for bit in (1, pair_bit, pair_bit | 1):
        pieces.append(swap(row_major(rows_of(me ^ bit)), bit, tp_size))
    return pieces


def solution(mesh):
    tp_size = mesh.shape['tp']
    x_bit, y_bit = 2, 4

    def device_step(x_blk, dy_blk, positions, norm_gain, wq_loc, wk_all, wv_all, wo_loc):
        heads = wq_loc.shape[1] // HEAD_DIM
        width = heads * HEAD_DIM
        rows, d_model = x_blk.shape
        me = lax.axis_index('tp')

        def head_of(weights, owner):
            return lax.dynamic_slice_in_dim(weights, owner * HEAD_DIM, HEAD_DIM, axis=1)

        wqkv = jnp.concatenate([wq_loc, head_of(wk_all, me), head_of(wv_all, me)], axis=1)

        x_f32 = x_blk.astype(F32)
        hidden, x_hat, inv_rms = norm_forward(x_f32, norm_gain)
        h_full = lax.all_gather(hidden, 'tp', axis=0, tiled=True)
        seq = h_full.shape[0]
        dy_in, h_full = lax.optimization_barrier((dy_blk, h_full))
        dy_full = lax.all_gather(dy_in, 'tp', axis=0, tiled=True)

        cos_t, sin_t = rope_tables(positions)
        doc_start = lax.iota(jnp.int32, seq) - positions
        lo = doc_start[::BQ] // BK
        full = (doc_start[BQ - 1::BQ] + BK - 1) // BK

        qkv = dot32(h_full, wqkv).astype(BF16)
        o, lse = attend_forward(lo, full, qkv, cos_t, sin_t, doc_start, heads)
        dy_full, o, wo_own, wq_own = lax.optimization_barrier((dy_full, o, wo_loc, wq_loc))
        wq_near = swap(wq_own, y_bit, tp_size)
        wo_near = swap(wo_own, x_bit, tp_size)
        o_pieces = group_rows(o.reshape(tp_size, rows, width), me, x_bit, y_bit, tp_size)

        d_o = dot32(dy_full, wo_loc, NT).astype(BF16)
        d_qkv = attend_backward(lo, full, qkv, o, d_o, lse, cos_t, sin_t, doc_start, heads)
        dq_pieces = group_rows(d_qkv.reshape(tp_size, rows, width + 2 * HEAD_DIM), me, y_bit, x_bit, tp_size)
        wq_near, wo_near, wq_own, wo_own, d_qkv = lax.optimization_barrier((wq_near, wo_near, wq_own, wo_own, d_qkv))
        wq_group = [wq_own, swap(wq_own, 1, tp_size), wq_near, swap(wq_near, 1, tp_size)]
        wo_group = [wo_own, swap(wo_own, 1, tp_size), wo_near, swap(wo_near, 1, tp_size)]

        d_wo = dot32(o, dy_full, TN).astype(BF16)
        d_wq = dot32(h_full, d_qkv[:, :width], TN).astype(BF16)
        d_wkv = dot32(h_full, d_qkv[:, width:], TN)
        dq_pieces, d_wo, d_wq, d_wkv = lax.optimization_barrier((dq_pieces, d_wo, d_wq, d_wkv))
        owners = jnp.stack([me ^ bit for bit in (0, 1, y_bit, y_bit | 1)])
        dh_mate = grad_mm(owners, dq_pieces, 1, wq_group, wk_all, wv_all, BF16)
        dh_got = swap(dh_mate, x_bit, tp_size)
        o_pieces, dh_mate = lax.optimization_barrier((o_pieces, dh_mate))
        mix_got = swap(mix_mm(o_pieces, 1, wo_group, BF16), y_bit, tp_size)
        dh_own = grad_mm(owners, dq_pieces, 0, wq_group, wk_all, wv_all, F32)
        mix_own = mix_mm(o_pieces, 0, wo_group, F32)

        d_wk, d_wv = d_wkv[:, :HEAD_DIM], d_wkv[:, HEAD_DIM:]
        d_f32 = (dh_own + dh_got.astype(F32)).astype(BF16).astype(F32)
        d_gain = sum_over_tp(jnp.sum(d_f32 * x_hat, axis=0), tp_size)
        scaled = d_f32 * norm_gain
        d_input = inv_rms * (scaled - x_hat * jnp.mean(scaled * x_hat, axis=-1, keepdims=True))
        grad_x = (dy_blk.astype(F32) + d_input).astype(BF16)
        result = (x_f32 + (mix_own + mix_got.astype(F32))).astype(BF16)
        return result, grad_x, d_wq, d_wk, d_wv, d_wo, d_gain

    specs_in = (P(('dp', 'tp'), None), P(('dp', 'tp'), None), P('dp'), P(), P(None, 'tp'), P(), P(), P('tp', None))
    specs_out = (P(('dp', 'tp'), None), P(('dp', 'tp'), None), P('dp', 'tp'), P('dp', 'tp'), P('dp', 'tp'), P(('dp', 'tp'), None), P('dp'))
    return jax.shard_map(device_step, mesh=mesh, in_specs=specs_in, out_specs=specs_out, check_vma=False)
```

```python
import functools
import jax
import jax.numpy as jnp
from jax import lax
from jax.experimental import pallas as pl
from jax.experimental.pallas import tpu as pltpu
from jax.experimental.layout import Layout, with_layout_constraint
from jax.sharding import PartitionSpec as P

HEAD_DIM = 128
SCORE_SCALE = HEAD_DIM ** -0.5
LOG2_SCALE = SCORE_SCALE * 1.4426950408889634
ROPE_THETA = 1000000.0
NORM_EPS = 1e-05
MASKED = -1e30
BQ = 256
BK = 512
VMEM_LIMIT = 60 * 1024 * 1024
NT = (((1,), (1,)), ((), ()))
TN = (((0,), (0,)), ((), ()))
F32 = jnp.float32
BF16 = jnp.bfloat16


def rope_tables(positions):
    exponents = jnp.arange(0, HEAD_DIM, 2, dtype=F32) / HEAD_DIM
    angles = positions.astype(F32)[..., None] * jnp.power(ROPE_THETA, -exponents)
    cos_t, sin_t = jnp.cos(angles), jnp.sin(angles)
    return jnp.concatenate([cos_t, cos_t], axis=-1), jnp.concatenate([-sin_t, sin_t], axis=-1)


def rope(x, cos_t, sin_t):
    x = x.astype(F32)
    return (x * cos_t + pltpu.roll(x, HEAD_DIM // 2, 1) * sin_t).astype(BF16)


def rope_back(x, cos_t, sin_t):
    x = x.astype(F32)
    return (x * cos_t - pltpu.roll(x, HEAD_DIM // 2, 1) * sin_t).astype(BF16)


def stack_heads(x, heads):
    return jnp.concatenate([x[:, h * HEAD_DIM:(h + 1) * HEAD_DIM] for h in range(heads)], axis=0)


def key_loops(i, lo_ref, full_ref, bq, bk, body):
    first = lo_ref[i]
    below = (i * bq) // bk
    last = ((i + 1) * bq + bk - 1) // bk
    mid = jnp.minimum(jnp.maximum(full_ref[i], first), last)
    mid_end = jnp.maximum(mid, jnp.minimum(below, last))
    lax.fori_loop(first, mid, functools.partial(body, True), None)
    lax.fori_loop(mid, mid_end, functools.partial(body, False), None)
    lax.fori_loop(mid_end, last, functools.partial(body, True), None)


def fwd_kernel(heads, lo_ref, full_ref, q_ref, k_ref, v_ref, cos_ref, sin_ref, cosf_ref, sinf_ref, ds_ref, o_ref, lse_ref, k_s, m_s, l_s, acc_s):
    i = pl.program_id(0)
    bq, bk = BQ, BK

    @pl.when(i == 0)
    def _():
        k_s[...] = rope(k_ref[...], cosf_ref[...], sinf_ref[...])

    cos_t, sin_t = cos_ref[...], sin_ref[...]
    q4 = jnp.concatenate([rope(q_ref[:, h * HEAD_DIM:(h + 1) * HEAD_DIM], cos_t, sin_t) for h in range(heads)], axis=0)
    m_s[...] = jnp.full_like(m_s, MASKED)
    l_s[...] = jnp.zeros_like(l_s)
    acc_s[...] = jnp.zeros_like(acc_s)

    def body(masked, j, _):
        start = pl.multiple_of(j * bk, bk)
        kj = k_s[pl.ds(start, bk), :]
        vj = v_ref[pl.ds(start, bk), :]
        s = lax.dot_general(q4, kj, NT, preferred_element_type=F32) * LOG2_SCALE
        if masked:
            q_idx = i * bq + lax.broadcasted_iota(jnp.int32, (bq, bk), 0)
            k_idx = start + lax.broadcasted_iota(jnp.int32, (bq, bk), 1)
            keep = (k_idx <= q_idx) & (k_idx >= ds_ref[...])
            s = jnp.concatenate([jnp.where(keep, s[h * bq:(h + 1) * bq], MASKED) for h in range(heads)], axis=0)
        m_prev = m_s[...]
        m_new = jnp.maximum(m_prev, jnp.max(s, axis=1, keepdims=True))
        p = jnp.exp2(s - jnp.tile(m_new, (1, bk // HEAD_DIM)))
        alpha = jnp.exp2(m_prev - m_new)
        l_s[...] = l_s[...] * alpha + jnp.sum(p, axis=1, keepdims=True)
        m_s[...] = m_new
        acc_s[...] = acc_s[...] * alpha + jnp.dot(p.astype(BF16), vj, preferred_element_type=F32)

    key_loops(i, lo_ref, full_ref, bq, bk, body)
    l_all = l_s[...]
    o4 = (acc_s[...] / l_all).astype(BF16)
    for h in range(heads):
        o_ref[:, h * HEAD_DIM:(h + 1) * HEAD_DIM] = o4[h * bq:(h + 1) * bq]
    lse = m_s[...] + jnp.log2(l_all)
    lse_ref[0] = lse.T[0:1, :]


def bwd_kernel(heads, n_blk, lo_ref, full_ref, q_ref, k_ref, v_ref, o_ref, do_ref, lse_ref, cos_ref, sin_ref, cosf_ref, sinf_ref, ds_ref, out_ref, k_s, dq_s, dk_s, dv_s):
    i = pl.program_id(0)
    bq, bk = BQ, BK
    width = heads * HEAD_DIM

    @pl.when(i == 0)
    def _():
        k_s[...] = rope(k_ref[...], cosf_ref[...], sinf_ref[...])
        dk_s[...] = jnp.zeros_like(dk_s)
        dv_s[...] = jnp.zeros_like(dv_s)

    cos_t, sin_t = cos_ref[...], sin_ref[...]
    q4 = jnp.concatenate([rope(q_ref[:, h * HEAD_DIM:(h + 1) * HEAD_DIM], cos_t, sin_t) for h in range(heads)], axis=0)
    do4 = stack_heads(do_ref[...], heads)
    o4 = stack_heads(o_ref[...], heads)
    delta = jnp.sum((do4.astype(F32) * o4.astype(F32)).T, axis=0, keepdims=True)
    lse = lse_ref[0]
    dq_s[...] = jnp.zeros_like(dq_s)

    def body(masked, j, _):
        start = pl.multiple_of(j * bk, bk)
        kj = k_s[pl.ds(start, bk), :]
        vj = v_ref[pl.ds(start, bk), :]
        s = lax.dot_general(kj, q4, NT, preferred_element_type=F32) * LOG2_SCALE
        if masked:
            q_idx = i * bq + lax.broadcasted_iota(jnp.int32, (bk, bq), 1)
            k_idx = start + lax.broadcasted_iota(jnp.int32, (bk, bq), 0)
            keep = (k_idx <= q_idx) & (k_idx >= ds_ref[0])
            s = jnp.concatenate([jnp.where(keep, s[:, h * bq:(h + 1) * bq], MASKED) for h in range(heads)], axis=1)
        p = jnp.exp2(s - lse)
        dp = lax.dot_general(vj, do4, NT, preferred_element_type=F32)
        dv_s[pl.ds(start, bk), :] += jnp.dot(p.astype(BF16), do4, preferred_element_type=F32)
        d_s = (p * (dp - delta)).astype(BF16)
        dk_s[pl.ds(start, bk), :] += jnp.dot(d_s, q4, preferred_element_type=F32)
        dq_s[...] += lax.dot_general(d_s, kj, TN, preferred_element_type=F32)

    key_loops(i, lo_ref, full_ref, bq, bk, body)
    row0 = pl.multiple_of(i * bq, bq)
    for h in range(heads):
        dq = (dq_s[h * bq:(h + 1) * bq, :] * SCORE_SCALE).astype(BF16)
        out_ref[pl.ds(row0, bq), h * HEAD_DIM:(h + 1) * HEAD_DIM] = rope_back(dq, cos_t, sin_t)

    @pl.when(i == n_blk - 1)
    def _():
        dk = (dk_s[...] * SCORE_SCALE).astype(BF16)
        out_ref[:, width:width + HEAD_DIM] = rope_back(dk, cosf_ref[...], sinf_ref[...])
        out_ref[:, width + HEAD_DIM:width + 2 * HEAD_DIM] = dv_s[...].astype(BF16)


def attention_specs(seq, heads):
    width = heads * HEAD_DIM
    q_spec = pl.BlockSpec((BQ, width), lambda i, *_: (i, 0))
    k_spec = pl.BlockSpec((seq, HEAD_DIM), lambda i, *_: (0, heads))
    v_spec = pl.BlockSpec((seq, HEAD_DIM), lambda i, *_: (0, heads + 1))
    tab_spec = pl.BlockSpec((BQ, HEAD_DIM), lambda i, *_: (i, 0))
    tabf_spec = pl.BlockSpec((seq, HEAD_DIM), lambda i, *_: (0, 0))
    row_spec = pl.BlockSpec((1, 1, heads * BQ), lambda i, *_: (i, 0, 0))
    return q_spec, k_spec, v_spec, tab_spec, tabf_spec, row_spec


def attend_forward(lo, full, qkv, cos_t, sin_t, doc_start, heads):
    seq = qkv.shape[0]
    n_blk = seq // BQ
    q_spec, k_spec, v_spec, tab_spec, tabf_spec, row_spec = attention_specs(seq, heads)
    return pl.pallas_call(
        functools.partial(fwd_kernel, heads),
        out_shape=(jax.ShapeDtypeStruct((seq, heads * HEAD_DIM), BF16), jax.ShapeDtypeStruct((n_blk, 1, heads * BQ), F32)),
        grid_spec=pltpu.PrefetchScalarGridSpec(
            num_scalar_prefetch=2, grid=(n_blk,),
            in_specs=[q_spec, k_spec, v_spec, tab_spec, tab_spec, tabf_spec, tabf_spec, pl.BlockSpec((BQ, 1), lambda i, *_: (i, 0))],
            out_specs=[q_spec, row_spec],
            scratch_shapes=[pltpu.VMEM((seq, HEAD_DIM), BF16)] + [pltpu.VMEM((heads * BQ, HEAD_DIM), F32)] * 3),
        compiler_params=pltpu.CompilerParams(dimension_semantics=("arbitrary",), vmem_limit_bytes=VMEM_LIMIT),
        cost_estimate=pl.CostEstimate(flops=4 * heads * seq * seq // 2 * HEAD_DIM, bytes_accessed=16 * 2 ** 20, transcendentals=heads * seq * seq // 2),
        name="attend_fwd",
    )(lo, full, qkv, qkv, qkv, cos_t, sin_t, cos_t, sin_t, doc_start[:, None])


def attend_backward(lo, full, qkv, o, d_o, lse, cos_t, sin_t, doc_start, heads):
    seq = qkv.shape[0]
    n_blk = seq // BQ
    width = heads * HEAD_DIM
    q_spec, k_spec, v_spec, tab_spec, tabf_spec, row_spec = attention_specs(seq, heads)
    return pl.pallas_call(
        functools.partial(bwd_kernel, heads, n_blk),
        out_shape=jax.ShapeDtypeStruct((seq, width + 2 * HEAD_DIM), BF16),
        grid_spec=pltpu.PrefetchScalarGridSpec(
            num_scalar_prefetch=2, grid=(n_blk,),
            in_specs=[q_spec, k_spec, v_spec, q_spec, q_spec, row_spec, tab_spec, tab_spec, tabf_spec, tabf_spec, pl.BlockSpec((1, 1, BQ), lambda i, *_: (i, 0, 0))],
            out_specs=pl.BlockSpec((seq, width + 2 * HEAD_DIM), lambda i, *_: (0, 0)),
            scratch_shapes=[pltpu.VMEM((seq, HEAD_DIM), BF16), pltpu.VMEM((heads * BQ, HEAD_DIM), F32), pltpu.VMEM((seq, HEAD_DIM), F32), pltpu.VMEM((seq, HEAD_DIM), F32)]),
        compiler_params=pltpu.CompilerParams(dimension_semantics=("arbitrary",), vmem_limit_bytes=VMEM_LIMIT),
        cost_estimate=pl.CostEstimate(flops=10 * heads * seq * seq // 2 * HEAD_DIM, bytes_accessed=24 * 2 ** 20, transcendentals=heads * seq * seq // 2),
        name="attend_bwd",
    )(lo, full, qkv, qkv, qkv, o, d_o, lse, cos_t, sin_t, cos_t, sin_t, doc_start.reshape(n_blk, 1, BQ))


def norm_forward(x_f32, norm_gain):
    inv_rms = lax.rsqrt(jnp.mean(x_f32 * x_f32, axis=-1, keepdims=True) + NORM_EPS)
    return (x_f32 * inv_rms * norm_gain).astype(BF16)


def dot32(a, b, dims=(((1,), (0,)), ((), ()))):
    return lax.dot_general(a, b, dims, preferred_element_type=F32)


def row_major(x):
    return with_layout_constraint(x, Layout(major_to_minor=tuple(range(x.ndim))))


def sum_over_tp(value, tp_size):
    step = 1
    while step < tp_size:
        value = value + lax.ppermute(value, 'tp', [(d, d ^ step) for d in range(tp_size)])
        step *= 2
    return value


def grad_mm_kernel(width, owner_ref, *refs):
    g_refs, w_refs, (wk_ref, wv_ref, out_ref, x_s, w_s) = refs[:4], refs[4:8], refs[8:]
    span = width + 2 * HEAD_DIM

    @pl.when(pl.program_id(0) == 0)
    def _():
        for p, g_ref in enumerate(g_refs):
            x_s[:, p * span:(p + 1) * span] = g_ref[0]

    for p, w_ref in enumerate(w_refs):
        head = pl.ds(pl.multiple_of(owner_ref[p] * HEAD_DIM, HEAD_DIM), HEAD_DIM)
        w_s[:, p * span:p * span + width] = w_ref[...]
        w_s[:, p * span + width:p * span + width + HEAD_DIM] = wk_ref[:, head]
        w_s[:, p * span + width + HEAD_DIM:(p + 1) * span] = wv_ref[:, head]
    out_ref[...] = lax.dot_general(x_s[...], w_s[...], NT, preferred_element_type=F32).astype(out_ref.dtype)


def grad_mm(owners, pieces, half, weights, wk_all, wv_all, dtype):
    _, rows, span = pieces[0].shape
    d_model, width = weights[0].shape
    bn = 512
    g_spec = pl.BlockSpec((1, rows, span), lambda j, *_: (half, 0, 0))
    w_spec = pl.BlockSpec((bn, width), lambda j, *_: (j, 0))
    kv_spec = pl.BlockSpec((bn, wk_all.shape[1]), lambda j, *_: (j, 0))
    return pl.pallas_call(
        functools.partial(grad_mm_kernel, width),
        out_shape=jax.ShapeDtypeStruct((rows, d_model), dtype),
        grid_spec=pltpu.PrefetchScalarGridSpec(
            num_scalar_prefetch=1, grid=(d_model // bn,),
            in_specs=[g_spec] * 4 + [w_spec] * 4 + [kv_spec] * 2,
            out_specs=pl.BlockSpec((rows, bn), lambda j, *_: (0, j)),
            scratch_shapes=[pltpu.VMEM((rows, 4 * span), BF16), pltpu.VMEM((bn, 4 * span), BF16)]),
        compiler_params=pltpu.CompilerParams(dimension_semantics=("arbitrary",), vmem_limit_bytes=VMEM_LIMIT),
        cost_estimate=pl.CostEstimate(flops=2 * rows * 4 * span * d_model, bytes_accessed=2 * (4 * span + 2 * rows) * d_model, transcendentals=0),
        name="grad_mm",
    )(owners, *pieces, *weights, wk_all, wv_all)


def mix_mm_kernel(width, *refs):
    o_refs, w_refs, (out_ref, x_s, w_s) = refs[:4], refs[4:8], refs[8:]

    @pl.when(pl.program_id(0) == 0)
    def _():
        for p, o_ref in enumerate(o_refs):
            x_s[:, p * width:(p + 1) * width] = o_ref[0]

    for p, w_ref in enumerate(w_refs):
        w_s[p * width:(p + 1) * width, :] = w_ref[...]
    out_ref[...] = jnp.dot(x_s[...], w_s[...], preferred_element_type=F32).astype(out_ref.dtype)


def mix_mm(pieces, half, weights, dtype):
    _, rows, width = pieces[0].shape
    d_model = weights[0].shape[1]
    bn = 512
    o_spec = pl.BlockSpec((1, rows, width), lambda j: (half, 0, 0))
    w_spec = pl.BlockSpec((width, bn), lambda j: (0, j))
    return pl.pallas_call(
        functools.partial(mix_mm_kernel, width),
        out_shape=jax.ShapeDtypeStruct((rows, d_model), dtype),
        grid=(d_model // bn,),
        in_specs=[o_spec] * 4 + [w_spec] * 4,
        out_specs=pl.BlockSpec((rows, bn), lambda j: (0, j)),
        scratch_shapes=[pltpu.VMEM((rows, 4 * width), BF16), pltpu.VMEM((4 * width, bn), BF16)],
        compiler_params=pltpu.CompilerParams(dimension_semantics=("arbitrary",), vmem_limit_bytes=VMEM_LIMIT),
        cost_estimate=pl.CostEstimate(flops=2 * rows * 4 * width * d_model, bytes_accessed=2 * (4 * width + 2 * rows) * d_model, transcendentals=0),
        name="mix_mm",
    )(*pieces, *weights)


def finish_kernel(own_ref, got_ref, x_ref, dy_ref, gain_ref, dx_ref, dg_ref):
    x = x_ref[...].astype(F32)
    inv_rms = lax.rsqrt(jnp.mean(x * x, axis=-1, keepdims=True) + NORM_EPS)
    x_hat = x * inv_rms
    d_hidden = (own_ref[...] + got_ref[...].astype(F32)).astype(BF16).astype(F32)

    @pl.when(pl.program_id(0) == 0)
    def _():
        dg_ref[...] = jnp.zeros_like(dg_ref)

    dg_ref[...] += jnp.sum(d_hidden * x_hat, axis=0, keepdims=True)
    scaled = d_hidden * gain_ref[...]
    d_input = inv_rms * (scaled - x_hat * jnp.mean(scaled * x_hat, axis=-1, keepdims=True))
    dx_ref[...] = (dy_ref[...].astype(F32) + d_input).astype(BF16)


def finish(dh_own, dh_got, x_blk, dy_blk, norm_gain):
    rows, d_model = x_blk.shape
    blk = pl.BlockSpec((64, d_model), lambda i: (i, 0))
    one = pl.BlockSpec((1, d_model), lambda i: (0, 0))
    grad_x, d_gain = pl.pallas_call(
        finish_kernel,
        out_shape=(jax.ShapeDtypeStruct((rows, d_model), BF16), jax.ShapeDtypeStruct((1, d_model), F32)),
        grid=(rows // 64,),
        in_specs=[blk, blk, blk, blk, one],
        out_specs=[blk, one],
        compiler_params=pltpu.CompilerParams(dimension_semantics=("arbitrary",), vmem_limit_bytes=VMEM_LIMIT),
        cost_estimate=pl.CostEstimate(flops=20 * rows * d_model, bytes_accessed=12 * rows * d_model, transcendentals=0),
        name="finish",
    )(dh_own, dh_got, x_blk, dy_blk, norm_gain[None, :])
    return grad_x, d_gain[0]


def swap(value, bit, tp_size):
    return lax.ppermute(value, 'tp', [(d, d ^ bit) for d in range(tp_size)])


def group_rows(blocks, me, pair_bit, mate_bit, tp_size):
    def rows_of(owner):
        return jnp.stack([lax.dynamic_index_in_dim(blocks, owner, 0, False), lax.dynamic_index_in_dim(blocks, owner ^ mate_bit, 0, False)])

    pieces = [rows_of(me)]
    for bit in (1, pair_bit, pair_bit | 1):
        pieces.append(swap(row_major(rows_of(me ^ bit)), bit, tp_size))
    return pieces


def solution(mesh):
    tp_size = mesh.shape['tp']
    x_bit, y_bit = 2, 4

    def layer(x_blk, dy_blk, positions, norm_gain, wq_loc, wk_all, wv_all, wo_loc):
        heads = wq_loc.shape[1] // HEAD_DIM
        width = heads * HEAD_DIM
        rows, _ = x_blk.shape
        me = lax.axis_index('tp')

        def head_of(weights, owner):
            return lax.dynamic_slice_in_dim(weights, owner * HEAD_DIM, HEAD_DIM, axis=1)

        wqkv = jnp.concatenate([wq_loc, head_of(wk_all, me), head_of(wv_all, me)], axis=1)

        x_f32 = x_blk.astype(F32)
        hidden = norm_forward(x_f32, norm_gain)
        h_full = lax.all_gather(hidden, 'tp', axis=0, tiled=True)
        seq = h_full.shape[0]
        dy_in, h_full = lax.optimization_barrier((dy_blk, h_full))
        dy_full = lax.all_gather(dy_in, 'tp', axis=0, tiled=True)

        cos_t, sin_t = rope_tables(positions)
        doc_start = lax.iota(jnp.int32, seq) - positions
        lo = doc_start[::BQ] // BK
        full = (doc_start[BQ - 1::BQ] + BK - 1) // BK

        qkv = dot32(h_full, wqkv).astype(BF16)
        o, lse = attend_forward(lo, full, qkv, cos_t, sin_t, doc_start, heads)
        dy_full, o, wo_own, wq_own = lax.optimization_barrier((dy_full, o, wo_loc, wq_loc))
        wq_near = swap(wq_own, y_bit, tp_size)
        wo_near = swap(wo_own, x_bit, tp_size)
        o_pieces = group_rows(o.reshape(tp_size, rows, width), me, x_bit, y_bit, tp_size)

        d_o = dot32(dy_full, wo_loc, NT).astype(BF16)
        d_qkv = attend_backward(lo, full, qkv, o, d_o, lse, cos_t, sin_t, doc_start, heads)
        dq_pieces = group_rows(d_qkv.reshape(tp_size, rows, width + 2 * HEAD_DIM), me, y_bit, x_bit, tp_size)
        wq_near, wq_own, d_qkv = lax.optimization_barrier((wq_near, wq_own, d_qkv))
        wq_group = [wq_own, swap(wq_own, 1, tp_size), wq_near, swap(wq_near, 1, tp_size)]

        d_wo = dot32(o, dy_full, TN).astype(BF16)
        d_wq = dot32(h_full, d_qkv[:, :width], TN).astype(BF16)
        d_wkv = dot32(h_full, d_qkv[:, width:], TN)
        wo_near, wo_own, d_wq = lax.optimization_barrier((wo_near, wo_own, d_wq))
        wo_group = [wo_own, swap(wo_own, 1, tp_size), wo_near, swap(wo_near, 1, tp_size)]
        mix_mate = mix_mm(o_pieces, 1, wo_group, BF16)
        dq_pieces, mix_mate, d_wq, d_wkv = lax.optimization_barrier((dq_pieces, mix_mate, d_wq, d_wkv))
        mix_got = swap(mix_mate, y_bit, tp_size)
        owners = jnp.stack([me ^ bit for bit in (0, 1, y_bit, y_bit | 1)])
        dh_mate = grad_mm(owners, dq_pieces, 1, wq_group, wk_all, wv_all, BF16)
        dh_got = swap(dh_mate, x_bit, tp_size)
        dh_own = grad_mm(owners, dq_pieces, 0, wq_group, wk_all, wv_all, F32)
        mix_own = mix_mm(o_pieces, 0, wo_group, F32)
        dh_own, dh_got, mix_own, d_wo = lax.optimization_barrier((dh_own, dh_got, mix_own, d_wo))

        d_wk, d_wv = d_wkv[:, :HEAD_DIM], d_wkv[:, HEAD_DIM:]
        grad_x, dg_part = finish(dh_own, dh_got, x_blk, dy_blk, norm_gain)
        d_gain = sum_over_tp(dg_part, tp_size)
        result = (x_f32 + (mix_own + mix_got.astype(F32))).astype(BF16)
        return result, grad_x, d_wq, d_wk, d_wv, d_wo, d_gain

    specs_in = (P(('dp', 'tp'), None), P(('dp', 'tp'), None), P('dp'), P(), P(None, 'tp'), P(), P(), P('tp', None))
    specs_out = (P(('dp', 'tp'), None), P(('dp', 'tp'), None), P('dp', 'tp'), P('dp', 'tp'), P('dp', 'tp'), P(('dp', 'tp'), None), P('dp'))
    return jax.shard_map(layer, mesh=mesh, in_specs=specs_in, out_specs=specs_out, check_vma=False)
```

```python
import functools
import jax
import jax.numpy as jnp
from jax import lax
from jax.experimental import pallas as pl
from jax.experimental.pallas import tpu as pltpu
from jax.sharding import PartitionSpec as P

HEAD_DIM = 128
SCORE_SCALE = HEAD_DIM ** -0.5
LOG2_SCALE = SCORE_SCALE * 1.4426950408889634
ROPE_THETA = 1000000.0
NORM_EPS = 1e-05
MASKED = -1e30
BQ = 256
BK = 512
VMEM_LIMIT = 60 * 1024 * 1024
NT = (((1,), (1,)), ((), ()))
TN = (((0,), (0,)), ((), ()))
F32 = jnp.float32
BF16 = jnp.bfloat16


def rope_tables(positions):
    exponents = jnp.arange(0, HEAD_DIM, 2, dtype=F32) / HEAD_DIM
    angles = positions.astype(F32)[..., None] * jnp.power(ROPE_THETA, -exponents)
    cos_t, sin_t = jnp.cos(angles), jnp.sin(angles)
    return jnp.concatenate([cos_t, cos_t], axis=-1), jnp.concatenate([-sin_t, sin_t], axis=-1)


def rope(x, cos_t, sin_t):
    x = x.astype(F32)
    return (x * cos_t + pltpu.roll(x, HEAD_DIM // 2, 1) * sin_t).astype(BF16)


def rope_back(x, cos_t, sin_t):
    x = x.astype(F32)
    return (x * cos_t - pltpu.roll(x, HEAD_DIM // 2, 1) * sin_t).astype(BF16)


def stack_heads(x, heads):
    return jnp.concatenate([x[:, h * HEAD_DIM:(h + 1) * HEAD_DIM] for h in range(heads)], axis=0)


def key_loops(i, lo_ref, full_ref, bq, bk, body):
    first = lo_ref[i]
    below = (i * bq) // bk
    last = ((i + 1) * bq + bk - 1) // bk
    mid = jnp.minimum(jnp.maximum(full_ref[i], first), last)
    mid_end = jnp.maximum(mid, jnp.minimum(below, last))
    lax.fori_loop(first, mid, functools.partial(body, True), None)
    lax.fori_loop(mid, mid_end, functools.partial(body, False), None)
    lax.fori_loop(mid_end, last, functools.partial(body, True), None)


def fwd_kernel(heads, lo_ref, full_ref, q_ref, k_ref, v_ref, cos_ref, sin_ref, cosf_ref, sinf_ref, ds_ref, o_ref, lse_ref, k_s, m_s, l_s, acc_s):
    i = pl.program_id(0)
    bq, bk = BQ, BK

    @pl.when(i == 0)
    def _():
        k_s[...] = rope(k_ref[...], cosf_ref[...], sinf_ref[...])

    cos_t, sin_t = cos_ref[...], sin_ref[...]
    q4 = jnp.concatenate([rope(q_ref[:, h * HEAD_DIM:(h + 1) * HEAD_DIM], cos_t, sin_t) for h in range(heads)], axis=0)
    m_s[...] = jnp.full_like(m_s, MASKED)
    l_s[...] = jnp.zeros_like(l_s)
    acc_s[...] = jnp.zeros_like(acc_s)

    def body(masked, j, _):
        start = pl.multiple_of(j * bk, bk)
        kj = k_s[pl.ds(start, bk), :]
        vj = v_ref[pl.ds(start, bk), :]
        s = lax.dot_general(q4, kj, NT, preferred_element_type=F32) * LOG2_SCALE
        if masked:
            q_idx = i * bq + lax.broadcasted_iota(jnp.int32, (bq, bk), 0)
            k_idx = start + lax.broadcasted_iota(jnp.int32, (bq, bk), 1)
            keep = (k_idx <= q_idx) & (k_idx >= ds_ref[...])
            s = jnp.concatenate([jnp.where(keep, s[h * bq:(h + 1) * bq], MASKED) for h in range(heads)], axis=0)
        m_prev = m_s[...]
        m_new = jnp.maximum(m_prev, jnp.max(s, axis=1, keepdims=True))
        p = jnp.exp2(s - jnp.tile(m_new, (1, bk // HEAD_DIM)))
        alpha = jnp.exp2(m_prev - m_new)
        l_s[...] = l_s[...] * alpha + jnp.sum(p, axis=1, keepdims=True)
        m_s[...] = m_new
        acc_s[...] = acc_s[...] * alpha + jnp.dot(p.astype(BF16), vj, preferred_element_type=F32)

    key_loops(i, lo_ref, full_ref, bq, bk, body)
    l_all = l_s[...]
    o4 = (acc_s[...] / l_all).astype(BF16)
    for h in range(heads):
        o_ref[:, h * HEAD_DIM:(h + 1) * HEAD_DIM] = o4[h * bq:(h + 1) * bq]
    lse = m_s[...] + jnp.log2(l_all)
    lse_ref[0] = lse.T[0:1, :]


def bwd_kernel(heads, half, parts, n_blk, lo_ref, full_ref, q_ref, k_ref, v_ref, o_ref, do_ref, lse_ref, cos_ref, sin_ref, cosf_ref, sinf_ref, ds_ref, *refs):
    first, last = half == 0, half == parts - 1
    if not first:
        refs = refs[1:]
        dk_in, dv_in = refs[:2]
        refs = refs[2:]
    if last:
        dq_ref, dkv_ref, k_s, dq_s, dk_s, dv_s = refs
    else:
        dq_ref, dk_s, dv_s, k_s, dq_s = refs
    step = pl.program_id(0)
    i = step * parts + half
    bq, bk = BQ, BK

    @pl.when(step == 0)
    def _():
        k_s[...] = rope(k_ref[...], cosf_ref[...], sinf_ref[...])
        dk_s[...] = jnp.zeros_like(dk_s) if first else dk_in[...]
        dv_s[...] = jnp.zeros_like(dv_s) if first else dv_in[...]

    cos_t, sin_t = cos_ref[...], sin_ref[...]
    q4 = jnp.concatenate([rope(q_ref[:, h * HEAD_DIM:(h + 1) * HEAD_DIM], cos_t, sin_t) for h in range(heads)], axis=0)
    do4 = stack_heads(do_ref[...], heads)
    o4 = stack_heads(o_ref[...], heads)
    delta = jnp.sum((do4.astype(F32) * o4.astype(F32)).T, axis=0, keepdims=True)
    lse = lse_ref[0]
    dq_s[...] = jnp.zeros_like(dq_s)

    def body(masked, j, _):
        start = pl.multiple_of(j * bk, bk)
        kj = k_s[pl.ds(start, bk), :]
        vj = v_ref[pl.ds(start, bk), :]
        s = lax.dot_general(kj, q4, NT, preferred_element_type=F32) * LOG2_SCALE
        if masked:
            q_idx = i * bq + lax.broadcasted_iota(jnp.int32, (bk, bq), 1)
            k_idx = start + lax.broadcasted_iota(jnp.int32, (bk, bq), 0)
            keep = (k_idx <= q_idx) & (k_idx >= ds_ref[0])
            s = jnp.concatenate([jnp.where(keep, s[:, h * bq:(h + 1) * bq], MASKED) for h in range(heads)], axis=1)
        p = jnp.exp2(s - lse)
        dp = lax.dot_general(vj, do4, NT, preferred_element_type=F32)
        dv_s[pl.ds(start, bk), :] += jnp.dot(p.astype(BF16), do4, preferred_element_type=F32)
        d_s = (p * (dp - delta)).astype(BF16)
        dk_s[pl.ds(start, bk), :] += jnp.dot(d_s, q4, preferred_element_type=F32)
        dq_s[...] += lax.dot_general(d_s, kj, TN, preferred_element_type=F32)

    key_loops(i, lo_ref, full_ref, bq, bk, body)
    for h in range(heads):
        dq = (dq_s[h * bq:(h + 1) * bq, :] * SCORE_SCALE).astype(BF16)
        dq_ref[:, h * HEAD_DIM:(h + 1) * HEAD_DIM] = rope_back(dq, cos_t, sin_t)

    if last:
        @pl.when(step == n_blk - 1)
        def _():
            dk = (dk_s[...] * SCORE_SCALE).astype(BF16)
            dkv_ref[:, :HEAD_DIM] = rope_back(dk, cosf_ref[...], sinf_ref[...])
            dkv_ref[:, HEAD_DIM:] = dv_s[...].astype(BF16)


def attention_specs(seq, heads):
    width = heads * HEAD_DIM
    q_spec = pl.BlockSpec((BQ, width), lambda i, *_: (i, 0))
    k_spec = pl.BlockSpec((seq, HEAD_DIM), lambda i, *_: (0, heads))
    v_spec = pl.BlockSpec((seq, HEAD_DIM), lambda i, *_: (0, heads + 1))
    tab_spec = pl.BlockSpec((BQ, HEAD_DIM), lambda i, *_: (i, 0))
    tabf_spec = pl.BlockSpec((seq, HEAD_DIM), lambda i, *_: (0, 0))
    row_spec = pl.BlockSpec((1, 1, heads * BQ), lambda i, *_: (i, 0, 0))
    return q_spec, k_spec, v_spec, tab_spec, tabf_spec, row_spec


def attend_forward(lo, full, qkv, cos_t, sin_t, doc_start, heads):
    seq = qkv.shape[0]
    n_blk = seq // BQ
    q_spec, k_spec, v_spec, tab_spec, tabf_spec, row_spec = attention_specs(seq, heads)
    return pl.pallas_call(
        functools.partial(fwd_kernel, heads),
        out_shape=(jax.ShapeDtypeStruct((seq, heads * HEAD_DIM), BF16), jax.ShapeDtypeStruct((n_blk, 1, heads * BQ), F32)),
        grid_spec=pltpu.PrefetchScalarGridSpec(
            num_scalar_prefetch=2, grid=(n_blk,),
            in_specs=[q_spec, k_spec, v_spec, tab_spec, tab_spec, tabf_spec, tabf_spec, pl.BlockSpec((BQ, 1), lambda i, *_: (i, 0))],
            out_specs=[q_spec, row_spec],
            scratch_shapes=[pltpu.VMEM((seq, HEAD_DIM), BF16)] + [pltpu.VMEM((heads * BQ, HEAD_DIM), F32)] * 3),
        compiler_params=pltpu.CompilerParams(dimension_semantics=("arbitrary",), vmem_limit_bytes=VMEM_LIMIT),
        cost_estimate=pl.CostEstimate(flops=4 * heads * seq * seq // 2 * HEAD_DIM, bytes_accessed=16 * 2 ** 20, transcendentals=heads * seq * seq // 2),
        name="attend_fwd",
    )(lo, full, qkv, qkv, qkv, cos_t, sin_t, cos_t, sin_t, doc_start[:, None])


def attend_backward(half, parts, carry, lo, full, qkv, o, d_o, lse, cos_t, sin_t, doc_start, heads):
    seq = qkv.shape[0]
    n_blk = seq // BQ // parts
    width = heads * HEAD_DIM
    _, k_spec, v_spec, _, full_spec, _ = attention_specs(seq, heads)
    q_spec = pl.BlockSpec((BQ, width), lambda i, *_: (i * parts + half, 0))
    do_spec = pl.BlockSpec((BQ, width), lambda i, *_: (i, 0))
    tab_spec = pl.BlockSpec((BQ, HEAD_DIM), lambda i, *_: (i * parts + half, 0))
    row_spec = pl.BlockSpec((1, 1, heads * BQ), lambda i, *_: (i * parts + half, 0, 0))
    ds_spec = pl.BlockSpec((1, 1, BQ), lambda i, *_: (i * parts + half, 0, 0))
    in_specs = [q_spec, k_spec, v_spec, q_spec, do_spec, row_spec, tab_spec, tab_spec, full_spec, full_spec, ds_spec]
    operands = [lo, full, qkv, qkv, qkv, o, d_o, lse, cos_t, sin_t, cos_t, sin_t, doc_start.reshape(seq // BQ, 1, BQ)]
    aliases = {}
    if half:
        aliases = {len(operands): 0}
        in_specs += [pl.BlockSpec(memory_space=pl.ANY), full_spec, full_spec]
        operands += list(carry)
    dq_shape = jax.ShapeDtypeStruct((seq, width), BF16)
    sum_shape = jax.ShapeDtypeStruct((seq, HEAD_DIM), F32)
    scratch = [pltpu.VMEM((seq, HEAD_DIM), BF16), pltpu.VMEM((heads * BQ, HEAD_DIM), F32)]
    if half == parts - 1:
        out_shape = (dq_shape, jax.ShapeDtypeStruct((seq, 2 * HEAD_DIM), BF16))
        out_specs = [q_spec, pl.BlockSpec((seq, 2 * HEAD_DIM), lambda i, *_: (0, 0))]
        scratch += [pltpu.VMEM((seq, HEAD_DIM), F32)] * 2
    else:
        out_shape = (dq_shape, sum_shape, sum_shape)
        out_specs = [q_spec, full_spec, full_spec]
    return pl.pallas_call(
        functools.partial(bwd_kernel, heads, half, parts, n_blk),
        out_shape=out_shape,
        grid_spec=pltpu.PrefetchScalarGridSpec(num_scalar_prefetch=2, grid=(n_blk,), in_specs=in_specs, out_specs=out_specs, scratch_shapes=scratch),
        input_output_aliases=aliases,
        compiler_params=pltpu.CompilerParams(dimension_semantics=("arbitrary",), vmem_limit_bytes=VMEM_LIMIT),
        cost_estimate=pl.CostEstimate(flops=10 * heads * seq * seq // 2 * HEAD_DIM // parts, bytes_accessed=24 * 2 ** 20 // parts, transcendentals=heads * seq * seq // 2 // parts),
    )(*operands)


def norm_forward(x_f32, norm_gain):
    inv_rms = lax.rsqrt(jnp.mean(x_f32 * x_f32, axis=-1, keepdims=True) + NORM_EPS)
    return (x_f32 * inv_rms * norm_gain).astype(BF16)


def dot32(a, b, dims=(((1,), (0,)), ((), ()))):
    return lax.dot_general(a, b, dims, preferred_element_type=F32)


def sum_over_tp(value, tp_size):
    step = 1
    while step < tp_size:
        value = value + lax.ppermute(value, 'tp', [(d, d ^ step) for d in range(tp_size)])
        step *= 2
    return value


def grad_mm_kernel(width, owner_ref, *refs):
    g_refs, w_refs, (wk_ref, wv_ref, out_ref, x_s, w_s) = refs[:4], refs[4:8], refs[8:]
    span = width + 2 * HEAD_DIM

    @pl.when(pl.program_id(0) == 0)
    def _():
        for p, g_ref in enumerate(g_refs):
            x_s[:, p * span:(p + 1) * span] = g_ref[0]

    for p, w_ref in enumerate(w_refs):
        head = pl.ds(pl.multiple_of(owner_ref[p] * HEAD_DIM, HEAD_DIM), HEAD_DIM)
        w_s[:, p * span:p * span + width] = w_ref[...]
        w_s[:, p * span + width:p * span + width + HEAD_DIM] = wk_ref[:, head]
        w_s[:, p * span + width + HEAD_DIM:(p + 1) * span] = wv_ref[:, head]
    out_ref[...] = lax.dot_general(x_s[...], w_s[...], NT, preferred_element_type=F32).astype(out_ref.dtype)


def grad_mm(owners, pieces, half, weights, wk_all, wv_all, dtype, part=0, parts=1):
    _, rows, span = pieces[0].shape
    rows = rows // parts
    d_model, width = weights[0].shape
    bn = 512
    g_spec = pl.BlockSpec((1, rows, span), lambda j, *_: (half, part, 0))
    w_spec = pl.BlockSpec((bn, width), lambda j, *_: (j, 0))
    kv_spec = pl.BlockSpec((bn, wk_all.shape[1]), lambda j, *_: (j, 0))
    return pl.pallas_call(
        functools.partial(grad_mm_kernel, width),
        out_shape=jax.ShapeDtypeStruct((rows, d_model), dtype),
        grid_spec=pltpu.PrefetchScalarGridSpec(
            num_scalar_prefetch=1, grid=(d_model // bn,),
            in_specs=[g_spec] * 4 + [w_spec] * 4 + [kv_spec] * 2,
            out_specs=pl.BlockSpec((rows, bn), lambda j, *_: (0, j)),
            scratch_shapes=[pltpu.VMEM((rows, 4 * span), BF16), pltpu.VMEM((bn, 4 * span), BF16)]),
        compiler_params=pltpu.CompilerParams(dimension_semantics=("arbitrary",), vmem_limit_bytes=VMEM_LIMIT),
        cost_estimate=pl.CostEstimate(flops=2 * rows * 4 * span * d_model, bytes_accessed=2 * (4 * span + 2 * rows) * d_model, transcendentals=0),
        name="grad_mm",
    )(owners, *pieces, *weights, wk_all, wv_all)


def mix_mm_kernel(width, *refs):
    o_refs, w_refs, (out_ref, x_s, w_s) = refs[:4], refs[4:8], refs[8:]

    @pl.when(pl.program_id(0) == 0)
    def _():
        for p, o_ref in enumerate(o_refs):
            x_s[:, p * width:(p + 1) * width] = o_ref[0]

    for p, w_ref in enumerate(w_refs):
        w_s[p * width:(p + 1) * width, :] = w_ref[...]
    out_ref[...] = jnp.dot(x_s[...], w_s[...], preferred_element_type=F32).astype(out_ref.dtype)


def mix_mm(pieces, half, weights, dtype):
    _, rows, width = pieces[0].shape
    d_model = weights[0].shape[1]
    bn = 512
    o_spec = pl.BlockSpec((1, rows, width), lambda j: (half, 0, 0))
    w_spec = pl.BlockSpec((width, bn), lambda j: (0, j))
    return pl.pallas_call(
        functools.partial(mix_mm_kernel, width),
        out_shape=jax.ShapeDtypeStruct((rows, d_model), dtype),
        grid=(d_model // bn,),
        in_specs=[o_spec] * 4 + [w_spec] * 4,
        out_specs=pl.BlockSpec((rows, bn), lambda j: (0, j)),
        scratch_shapes=[pltpu.VMEM((rows, 4 * width), BF16), pltpu.VMEM((4 * width, bn), BF16)],
        compiler_params=pltpu.CompilerParams(dimension_semantics=("arbitrary",), vmem_limit_bytes=VMEM_LIMIT),
        cost_estimate=pl.CostEstimate(flops=2 * rows * 4 * width * d_model, bytes_accessed=2 * (4 * width + 2 * rows) * d_model, transcendentals=0),
        name="mix_mm",
    )(*pieces, *weights)


def finish_kernel(part, own_ref, got_ref, x_ref, dy_ref, gain_ref, *refs):
    dx_ref, dg_ref = refs[-2:]
    x = x_ref[...].astype(F32)
    inv_rms = lax.rsqrt(jnp.mean(x * x, axis=-1, keepdims=True) + NORM_EPS)
    x_hat = x * inv_rms
    d_hidden = (own_ref[...] + got_ref[...].astype(F32)).astype(BF16).astype(F32)

    @pl.when(pl.program_id(0) == 0)
    def _():
        dg_ref[...] = refs[1][...] if part else jnp.zeros_like(dg_ref)

    dg_ref[...] += jnp.sum(d_hidden * x_hat, axis=0, keepdims=True)
    scaled = d_hidden * gain_ref[...]
    d_input = inv_rms * (scaled - x_hat * jnp.mean(scaled * x_hat, axis=-1, keepdims=True))
    dx_ref[...] = (dy_ref[...].astype(F32) + d_input).astype(BF16)


def finish(part, parts, carry, dh_own, dh_got, x_blk, dy_blk, norm_gain):
    rows, d_model = x_blk.shape
    blk_rows = 64
    steps = rows // parts // blk_rows
    blk = pl.BlockSpec((blk_rows, d_model), lambda i: (i + part * steps, 0))
    got = pl.BlockSpec((blk_rows, d_model), lambda i: (i, 0))
    one = pl.BlockSpec((1, d_model), lambda i: (0, 0))
    operands = [dh_own, dh_got, x_blk, dy_blk, norm_gain[None, :]]
    in_specs = [blk, got, blk, blk, one]
    aliases = {}
    if part:
        aliases = {5: 0}
        operands += list(carry)
        in_specs += [pl.BlockSpec(memory_space=pl.ANY), one]
    return pl.pallas_call(
        functools.partial(finish_kernel, part),
        out_shape=(jax.ShapeDtypeStruct((rows, d_model), BF16), jax.ShapeDtypeStruct((1, d_model), F32)),
        grid=(steps,),
        in_specs=in_specs,
        out_specs=[blk, one],
        input_output_aliases=aliases,
        compiler_params=pltpu.CompilerParams(dimension_semantics=("arbitrary",), vmem_limit_bytes=VMEM_LIMIT),
        cost_estimate=pl.CostEstimate(flops=20 * rows * d_model // parts, bytes_accessed=12 * rows * d_model // parts, transcendentals=0),
    )(*operands)


def swap(value, bit, tp_size):
    return lax.ppermute(value, 'tp', [(d, d ^ bit) for d in range(tp_size)])


def pack_kernel(n_in, owner_ref, *refs):
    ins, outs = refs[:4 * n_in], refs[4 * n_in:]
    for p, out_ref in enumerate(outs):
        at = 0
        for ref in ins[p * n_in:(p + 1) * n_in]:
            out_ref[0, :, at:at + ref.shape[2]] = ref[0]
            at += ref.shape[2]


def group_rows(blocks, me, pair_bit, mate_bit, tp_size):
    bits = (0, 1, pair_bit, pair_bit | 1)
    owners = jnp.stack([me ^ bit ^ mate for bit in bits for mate in (0, mate_bit)])
    rows = blocks[0].shape[1]
    span = sum(b.shape[2] for b in blocks)
    in_specs = [pl.BlockSpec((1, rows, b.shape[2]), functools.partial(lambda p, h, owner: (owner[2 * p + h], 0, 0), p)) for p in range(4) for b in blocks]
    sent = pl.pallas_call(
        functools.partial(pack_kernel, len(blocks)),
        out_shape=[jax.ShapeDtypeStruct((2, rows, span), BF16)] * 4,
        grid_spec=pltpu.PrefetchScalarGridSpec(num_scalar_prefetch=1, grid=(2,), in_specs=in_specs,
                                               out_specs=[pl.BlockSpec((1, rows, span), lambda h, owner: (h, 0, 0))] * 4),
        compiler_params=pltpu.CompilerParams(dimension_semantics=("arbitrary",), vmem_limit_bytes=VMEM_LIMIT),
        cost_estimate=pl.CostEstimate(flops=0, bytes_accessed=32 * rows * span, transcendentals=0),
        name="pack_rows",
    )(owners, *(list(blocks) * 4))
    pieces = [sent[0]]
    for bit, rows_sent in zip(bits[1:], sent[1:]):
        pieces.append(swap(rows_sent, bit, tp_size))
    return pieces


def solution(mesh):
    tp_size = mesh.shape['tp']
    x_bit, y_bit = 2, 4

    def layer(x_blk, dy_blk, positions, norm_gain, wq_loc, wk_all, wv_all, wo_loc):
        heads = wq_loc.shape[1] // HEAD_DIM
        width = heads * HEAD_DIM
        rows, _ = x_blk.shape
        me = lax.axis_index('tp')

        def head_of(weights, owner):
            return lax.dynamic_slice_in_dim(weights, owner * HEAD_DIM, HEAD_DIM, axis=1)

        wqkv = jnp.concatenate([wq_loc, head_of(wk_all, me), head_of(wv_all, me)], axis=1)

        x_f32 = x_blk.astype(F32)
        hidden = norm_forward(x_f32, norm_gain)
        h_full = lax.all_gather(hidden, 'tp', axis=0, tiled=True)
        seq = h_full.shape[0]
        parts = rows // BQ
        dy_late, _ = lax.optimization_barrier((dy_blk, hidden))
        dy_in = [dy_late[p * BQ:(p + 1) * BQ] for p in range(parts)]
        dy_full = [lax.all_gather(dy_in[0], 'tp', axis=0, tiled=True)]

        cos_t, sin_t = rope_tables(positions)
        doc_start = lax.iota(jnp.int32, seq) - positions
        lo = doc_start[::BQ] // BK
        full = (doc_start[BQ - 1::BQ] + BK - 1) // BK

        qkv = dot32(h_full, wqkv).astype(BF16)
        *dy_rest, qkv = lax.optimization_barrier((*dy_in[1:], qkv))
        dy_full += [lax.all_gather(dy_part, 'tp', axis=0, tiled=True) for dy_part in dy_rest]
        o, lse = attend_forward(lo, full, qkv, cos_t, sin_t, doc_start, heads)
        dy_full[0], o = lax.optimization_barrier((dy_full[0], o))
        o_blocks = o.reshape(tp_size, parts, BQ, width)
        carry = None
        for p in range(parts - 1):
            d_o = dot32(dy_full[p], wo_loc, NT).astype(BF16)
            carry = attend_backward(p, parts, carry, lo, full, qkv, o, d_o, lse, cos_t, sin_t, doc_start, heads)
        dy_full[-1], o_sent, wo_own, wq_own = lax.optimization_barrier((dy_full[-1], o, wo_loc, wq_loc))
        wq_near = swap(wq_own, y_bit, tp_size)
        wo_near = swap(wo_own, x_bit, tp_size)
        o_pieces = group_rows([o_sent.reshape(tp_size, rows, width)], me, x_bit, y_bit, tp_size)

        d_o = dot32(dy_full[-1], wo_loc, NT).astype(BF16)
        d_q, d_kv = attend_backward(parts - 1, parts, carry, lo, full, qkv, o, d_o, lse, cos_t, sin_t, doc_start, heads)
        dq_pieces = group_rows([d_q.reshape(tp_size, rows, width), d_kv.reshape(tp_size, rows, 2 * HEAD_DIM)], me, y_bit, x_bit, tp_size)
        d_wq = dot32(h_full, d_q, TN).astype(BF16)
        d_wkv = dot32(h_full, d_kv, TN)
        wq_near, wq_own, d_wq, d_wkv = lax.optimization_barrier((wq_near, wq_own, d_wq, d_wkv))
        wq_side = swap(wq_own, 1, tp_size)
        wq_group = [wq_own, wq_side, wq_near, swap(wq_near, 1, tp_size)]
        o_blocks, d_wkv = lax.optimization_barrier((o_blocks, d_wkv))
        d_wo = dot32(o_blocks[:, 0].reshape(-1, width), dy_full[0], TN)
        d_wo = (d_wo + sum(dot32(o_blocks[:, p].reshape(-1, width), dy_full[p], TN) for p in range(1, parts))).astype(BF16)
        wo_near, wo_own, d_wo = lax.optimization_barrier((wo_near, wo_own, d_wo))
        wo_group = [wo_own, swap(wo_own, 1, tp_size), wo_near, swap(wo_near, 1, tp_size)]
        mix_mate = mix_mm(o_pieces, 1, wo_group, BF16)
        dq_pieces, mix_mate, d_wq, d_wkv = lax.optimization_barrier((dq_pieces, mix_mate, d_wq, d_wkv))
        mix_got = swap(mix_mate, y_bit, tp_size)
        owners = jnp.stack([me ^ bit for bit in (0, 1, y_bit, y_bit | 1)])
        halves = 2
        dh_got = []
        for p in range(halves):
            dh_mate = grad_mm(owners, dq_pieces, 1, wq_group, wk_all, wv_all, BF16, p, halves)
            dh_got.append(swap(dh_mate, x_bit, tp_size))
        dh_own = grad_mm(owners, dq_pieces, 0, wq_group, wk_all, wv_all, F32)
        mix_own = mix_mm(o_pieces, 0, wo_group, F32)
        result = (x_f32 + (mix_own + mix_got.astype(F32))).astype(BF16)
        d_wk, d_wv = d_wkv[:, :HEAD_DIM], d_wkv[:, HEAD_DIM:]
        dh_own, dh_got[0], result, d_wo, d_wk, d_wv = lax.optimization_barrier((dh_own, dh_got[0], result, d_wo, d_wk, d_wv))
        done = None
        for p in range(halves):
            done = finish(p, halves, done, dh_own, dh_got[p], x_blk, dy_blk, norm_gain)
        grad_x, d_gain = done[0], sum_over_tp(done[1][0], tp_size)
        return result, grad_x, d_wq, d_wk, d_wv, d_wo, d_gain

    specs_in = (P(('dp', 'tp'), None), P(('dp', 'tp'), None), P('dp'), P(), P(None, 'tp'), P(), P(), P('tp', None))
    specs_out = (P(('dp', 'tp'), None), P(('dp', 'tp'), None), P('dp', 'tp'), P('dp', 'tp'), P('dp', 'tp'), P(('dp', 'tp'), None), P('dp'))
    return jax.shard_map(layer, mesh=mesh, in_specs=specs_in, out_specs=specs_out, check_vma=False)
```

```python
import functools
import jax
import jax.numpy as jnp
from jax import lax
from jax.experimental import pallas as pl
from jax.experimental.pallas import tpu as pltpu
from jax.sharding import PartitionSpec as P

HEAD_DIM = 128
SCORE_SCALE = HEAD_DIM ** -0.5
LOG2_SCALE = SCORE_SCALE * 1.4426950408889634
ROPE_THETA = 1000000.0
NORM_EPS = 1e-05
MASKED = -1e30
BQ = 256
BK = 512
VMEM_LIMIT = 60 * 1024 * 1024
NT = (((1,), (1,)), ((), ()))
TN = (((0,), (0,)), ((), ()))
F32 = jnp.float32
BF16 = jnp.bfloat16


def rope_tables(positions):
    exponents = jnp.arange(0, HEAD_DIM, 2, dtype=F32) / HEAD_DIM
    angles = positions.astype(F32)[..., None] * jnp.power(ROPE_THETA, -exponents)
    cos_t, sin_t = jnp.cos(angles), jnp.sin(angles)
    return jnp.concatenate([cos_t, cos_t], axis=-1), jnp.concatenate([-sin_t, sin_t], axis=-1)


def rope(x, cos_t, sin_t):
    x = x.astype(F32)
    return (x * cos_t + pltpu.roll(x, HEAD_DIM // 2, 1) * sin_t).astype(BF16)


def rope_back(x, cos_t, sin_t):
    x = x.astype(F32)
    return (x * cos_t - pltpu.roll(x, HEAD_DIM // 2, 1) * sin_t).astype(BF16)


def stack_heads(x, heads):
    return jnp.concatenate([x[:, h * HEAD_DIM:(h + 1) * HEAD_DIM] for h in range(heads)], axis=0)


def key_loops(i, lo_ref, full_ref, bq, bk, body):
    first = lo_ref[i]
    below = (i * bq) // bk
    last = ((i + 1) * bq + bk - 1) // bk
    mid = jnp.minimum(jnp.maximum(full_ref[i], first), last)
    mid_end = jnp.maximum(mid, jnp.minimum(below, last))
    lax.fori_loop(first, mid, functools.partial(body, True), None)
    lax.fori_loop(mid, mid_end, functools.partial(body, False), None)
    lax.fori_loop(mid_end, last, functools.partial(body, True), None)


def fwd_kernel(heads, lo_ref, full_ref, q_ref, k_ref, v_ref, cos_ref, sin_ref, cosf_ref, sinf_ref, ds_ref, o_ref, lse_ref, k_s, m_s, l_s, acc_s):
    i = pl.program_id(0)
    bq, bk = BQ, BK

    @pl.when(i == 0)
    def _():
        k_s[...] = rope(k_ref[...], cosf_ref[...], sinf_ref[...])

    cos_t, sin_t = cos_ref[...], sin_ref[...]
    q4 = jnp.concatenate([rope(q_ref[:, h * HEAD_DIM:(h + 1) * HEAD_DIM], cos_t, sin_t) for h in range(heads)], axis=0)
    m_s[...] = jnp.full_like(m_s, MASKED)
    l_s[...] = jnp.zeros_like(l_s)
    acc_s[...] = jnp.zeros_like(acc_s)

    def body(masked, j, _):
        start = pl.multiple_of(j * bk, bk)
        kj = k_s[pl.ds(start, bk), :]
        vj = v_ref[pl.ds(start, bk), :]
        s = lax.dot_general(q4, kj, NT, preferred_element_type=F32) * LOG2_SCALE
        if masked:
            q_idx = i * bq + lax.broadcasted_iota(jnp.int32, (bq, bk), 0)
            k_idx = start + lax.broadcasted_iota(jnp.int32, (bq, bk), 1)
            keep = (k_idx <= q_idx) & (k_idx >= ds_ref[...])
            s = jnp.concatenate([jnp.where(keep, s[h * bq:(h + 1) * bq], MASKED) for h in range(heads)], axis=0)
        m_prev = m_s[...]
        m_new = jnp.maximum(m_prev, jnp.max(s, axis=1, keepdims=True))
        p = jnp.exp2(s - jnp.tile(m_new, (1, bk // HEAD_DIM)))
        alpha = jnp.exp2(m_prev - m_new)
        l_s[...] = l_s[...] * alpha + jnp.sum(p, axis=1, keepdims=True)
        m_s[...] = m_new
        acc_s[...] = acc_s[...] * alpha + jnp.dot(p.astype(BF16), vj, preferred_element_type=F32)

    key_loops(i, lo_ref, full_ref, bq, bk, body)
    l_all = l_s[...]
    o4 = (acc_s[...] / l_all).astype(BF16)
    for h in range(heads):
        o_ref[:, h * HEAD_DIM:(h + 1) * HEAD_DIM] = o4[h * bq:(h + 1) * bq]
    lse = m_s[...] + jnp.log2(l_all)
    lse_ref[0] = lse.T[0:1, :]


def bwd_kernel(heads, half, parts, n_blk, lo_ref, full_ref, q_ref, k_ref, v_ref, o_ref, do_ref, lse_ref, cos_ref, sin_ref, cosf_ref, sinf_ref, ds_ref, *refs):
    first, last = half == 0, half == parts - 1
    if not first:
        refs = refs[1:]
        dk_in, dv_in = refs[:2]
        refs = refs[2:]
    if last:
        dq_ref, dkv_ref, k_s, dq_s, dk_s, dv_s = refs
    else:
        dq_ref, dk_s, dv_s, k_s, dq_s = refs
    step = pl.program_id(0)
    i = step * parts + half
    bq, bk = BQ, BK

    @pl.when(step == 0)
    def _():
        k_s[...] = rope(k_ref[...], cosf_ref[...], sinf_ref[...])
        dk_s[...] = jnp.zeros_like(dk_s) if first else dk_in[...]
        dv_s[...] = jnp.zeros_like(dv_s) if first else dv_in[...]

    cos_t, sin_t = cos_ref[...], sin_ref[...]
    q4 = jnp.concatenate([rope(q_ref[:, h * HEAD_DIM:(h + 1) * HEAD_DIM], cos_t, sin_t) for h in range(heads)], axis=0)
    do4 = stack_heads(do_ref[...], heads)
    o4 = stack_heads(o_ref[...], heads)
    delta = jnp.sum((do4.astype(F32) * o4.astype(F32)).T, axis=0, keepdims=True)
    lse = lse_ref[0]
    dq_s[...] = jnp.zeros_like(dq_s)

    def body(masked, j, _):
        start = pl.multiple_of(j * bk, bk)
        kj = k_s[pl.ds(start, bk), :]
        vj = v_ref[pl.ds(start, bk), :]
        s = lax.dot_general(kj, q4, NT, preferred_element_type=F32) * LOG2_SCALE
        if masked:
            q_idx = i * bq + lax.broadcasted_iota(jnp.int32, (bk, bq), 1)
            k_idx = start + lax.broadcasted_iota(jnp.int32, (bk, bq), 0)
            keep = (k_idx <= q_idx) & (k_idx >= ds_ref[0])
            s = jnp.concatenate([jnp.where(keep, s[:, h * bq:(h + 1) * bq], MASKED) for h in range(heads)], axis=1)
        p = jnp.exp2(s - lse)
        dp = lax.dot_general(vj, do4, NT, preferred_element_type=F32)
        dv_s[pl.ds(start, bk), :] += jnp.dot(p.astype(BF16), do4, preferred_element_type=F32)
        d_s = (p * (dp - delta)).astype(BF16)
        dk_s[pl.ds(start, bk), :] += jnp.dot(d_s, q4, preferred_element_type=F32)
        dq_s[...] += lax.dot_general(d_s, kj, TN, preferred_element_type=F32)

    key_loops(i, lo_ref, full_ref, bq, bk, body)
    for h in range(heads):
        dq = (dq_s[h * bq:(h + 1) * bq, :] * SCORE_SCALE).astype(BF16)
        dq_ref[:, h * HEAD_DIM:(h + 1) * HEAD_DIM] = rope_back(dq, cos_t, sin_t)

    if last:
        @pl.when(step == n_blk - 1)
        def _():
            dk = (dk_s[...] * SCORE_SCALE).astype(BF16)
            dkv_ref[:, :HEAD_DIM] = rope_back(dk, cosf_ref[...], sinf_ref[...])
            dkv_ref[:, HEAD_DIM:] = dv_s[...].astype(BF16)


def attention_specs(seq, heads):
    width = heads * HEAD_DIM
    q_spec = pl.BlockSpec((BQ, width), lambda i, *_: (i, 0))
    k_spec = pl.BlockSpec((seq, HEAD_DIM), lambda i, *_: (0, heads))
    v_spec = pl.BlockSpec((seq, HEAD_DIM), lambda i, *_: (0, heads + 1))
    tab_spec = pl.BlockSpec((BQ, HEAD_DIM), lambda i, *_: (i, 0))
    tabf_spec = pl.BlockSpec((seq, HEAD_DIM), lambda i, *_: (0, 0))
    row_spec = pl.BlockSpec((1, 1, heads * BQ), lambda i, *_: (i, 0, 0))
    return q_spec, k_spec, v_spec, tab_spec, tabf_spec, row_spec


def attend_forward(lo, full, qkv, cos_t, sin_t, doc_start, heads):
    seq = qkv.shape[0]
    n_blk = seq // BQ
    q_spec, k_spec, v_spec, tab_spec, tabf_spec, row_spec = attention_specs(seq, heads)
    return pl.pallas_call(
        functools.partial(fwd_kernel, heads),
        out_shape=(jax.ShapeDtypeStruct((seq, heads * HEAD_DIM), BF16), jax.ShapeDtypeStruct((n_blk, 1, heads * BQ), F32)),
        grid_spec=pltpu.PrefetchScalarGridSpec(
            num_scalar_prefetch=2, grid=(n_blk,),
            in_specs=[q_spec, k_spec, v_spec, tab_spec, tab_spec, tabf_spec, tabf_spec, pl.BlockSpec((BQ, 1), lambda i, *_: (i, 0))],
            out_specs=[q_spec, row_spec],
            scratch_shapes=[pltpu.VMEM((seq, HEAD_DIM), BF16)] + [pltpu.VMEM((heads * BQ, HEAD_DIM), F32)] * 3),
        compiler_params=pltpu.CompilerParams(dimension_semantics=("arbitrary",), vmem_limit_bytes=VMEM_LIMIT),
        cost_estimate=pl.CostEstimate(flops=4 * heads * seq * seq // 2 * HEAD_DIM, bytes_accessed=16 * 2 ** 20, transcendentals=heads * seq * seq // 2),
        name="attend_fwd",
    )(lo, full, qkv, qkv, qkv, cos_t, sin_t, cos_t, sin_t, doc_start[:, None])


def attend_backward(half, parts, carry, lo, full, qkv, o, d_o, lse, cos_t, sin_t, doc_start, heads):
    seq = qkv.shape[0]
    n_blk = seq // BQ // parts
    width = heads * HEAD_DIM
    _, k_spec, v_spec, _, full_spec, _ = attention_specs(seq, heads)
    q_spec = pl.BlockSpec((BQ, width), lambda i, *_: (i * parts + half, 0))
    do_spec = pl.BlockSpec((BQ, width), lambda i, *_: (i, 0))
    tab_spec = pl.BlockSpec((BQ, HEAD_DIM), lambda i, *_: (i * parts + half, 0))
    row_spec = pl.BlockSpec((1, 1, heads * BQ), lambda i, *_: (i * parts + half, 0, 0))
    ds_spec = pl.BlockSpec((1, 1, BQ), lambda i, *_: (i * parts + half, 0, 0))
    in_specs = [q_spec, k_spec, v_spec, q_spec, do_spec, row_spec, tab_spec, tab_spec, full_spec, full_spec, ds_spec]
    operands = [lo, full, qkv, qkv, qkv, o, d_o, lse, cos_t, sin_t, cos_t, sin_t, doc_start.reshape(seq // BQ, 1, BQ)]
    aliases = {}
    if half:
        aliases = {len(operands): 0}
        in_specs += [pl.BlockSpec(memory_space=pl.ANY), full_spec, full_spec]
        operands += list(carry)
    dq_shape = jax.ShapeDtypeStruct((seq, width), BF16)
    sum_shape = jax.ShapeDtypeStruct((seq, HEAD_DIM), F32)
    scratch = [pltpu.VMEM((seq, HEAD_DIM), BF16), pltpu.VMEM((heads * BQ, HEAD_DIM), F32)]
    if half == parts - 1:
        out_shape = (dq_shape, jax.ShapeDtypeStruct((seq, 2 * HEAD_DIM), BF16))
        out_specs = [q_spec, pl.BlockSpec((seq, 2 * HEAD_DIM), lambda i, *_: (0, 0))]
        scratch += [pltpu.VMEM((seq, HEAD_DIM), F32)] * 2
    else:
        out_shape = (dq_shape, sum_shape, sum_shape)
        out_specs = [q_spec, full_spec, full_spec]
    return pl.pallas_call(
        functools.partial(bwd_kernel, heads, half, parts, n_blk),
        out_shape=out_shape,
        grid_spec=pltpu.PrefetchScalarGridSpec(num_scalar_prefetch=2, grid=(n_blk,), in_specs=in_specs, out_specs=out_specs, scratch_shapes=scratch),
        input_output_aliases=aliases,
        compiler_params=pltpu.CompilerParams(dimension_semantics=("arbitrary",), vmem_limit_bytes=VMEM_LIMIT),
        cost_estimate=pl.CostEstimate(flops=10 * heads * seq * seq // 2 * HEAD_DIM // parts, bytes_accessed=24 * 2 ** 20 // parts, transcendentals=heads * seq * seq // 2 // parts),
    )(*operands)


def norm_forward(x_f32, norm_gain):
    inv_rms = lax.rsqrt(jnp.mean(x_f32 * x_f32, axis=-1, keepdims=True) + NORM_EPS)
    return (x_f32 * inv_rms * norm_gain).astype(BF16)


def dot32(a, b, dims=(((1,), (0,)), ((), ()))):
    return lax.dot_general(a, b, dims, preferred_element_type=F32)


def sum_over_tp(value, tp_size):
    step = 1
    while step < tp_size:
        value = value + lax.ppermute(value, 'tp', [(d, d ^ step) for d in range(tp_size)])
        step *= 2
    return value


def grad_mm_kernel(width, owner_ref, *refs):
    g_refs, w_refs, (wk_ref, wv_ref, *out_refs, x_s, w_s) = refs[:4], refs[4:8], refs[8:]
    span = width + 2 * HEAD_DIM

    @pl.when(pl.program_id(0) == 0)
    def _():
        for p, g_ref in enumerate(g_refs):
            x_s[:, p * span:(p + 1) * span] = g_ref[0]

    for p, w_ref in enumerate(w_refs):
        head = pl.ds(pl.multiple_of(owner_ref[p] * HEAD_DIM, HEAD_DIM), HEAD_DIM)
        w_s[:, p * span:p * span + width] = w_ref[...]
        w_s[:, p * span + width:p * span + width + HEAD_DIM] = wk_ref[:, head]
        w_s[:, p * span + width + HEAD_DIM:(p + 1) * span] = wv_ref[:, head]
    out = lax.dot_general(x_s[...], w_s[...], NT, preferred_element_type=F32)
    rows = out_refs[0].shape[0]
    for r, out_ref in enumerate(out_refs):
        out_ref[...] = out[r * rows:(r + 1) * rows].astype(out_ref.dtype)


def grad_mm(owners, pieces, half, weights, wk_all, wv_all, dtype, parts=1):
    _, rows, span = pieces[0].shape
    d_model, width = weights[0].shape
    bn = 512
    g_spec = pl.BlockSpec((1, rows, span), lambda j, *_: (half, 0, 0))
    w_spec = pl.BlockSpec((bn, width), lambda j, *_: (j, 0))
    kv_spec = pl.BlockSpec((bn, wk_all.shape[1]), lambda j, *_: (j, 0))
    return pl.pallas_call(
        functools.partial(grad_mm_kernel, width),
        out_shape=[jax.ShapeDtypeStruct((rows // parts, d_model), dtype)] * parts,
        grid_spec=pltpu.PrefetchScalarGridSpec(
            num_scalar_prefetch=1, grid=(d_model // bn,),
            in_specs=[g_spec] * 4 + [w_spec] * 4 + [kv_spec] * 2,
            out_specs=[pl.BlockSpec((rows // parts, bn), lambda j, *_: (0, j))] * parts,
            scratch_shapes=[pltpu.VMEM((rows, 4 * span), BF16), pltpu.VMEM((bn, 4 * span), BF16)]),
        compiler_params=pltpu.CompilerParams(dimension_semantics=("arbitrary",), vmem_limit_bytes=VMEM_LIMIT),
        cost_estimate=pl.CostEstimate(flops=2 * rows * 4 * span * d_model, bytes_accessed=2 * (4 * span + 2 * rows) * d_model, transcendentals=0),
        name="grad_mm",
    )(owners, *pieces, *weights, wk_all, wv_all)


def mix_mm_kernel(width, *refs):
    o_refs, w_refs, (*add_refs, out_ref, x_s, w_s) = refs[:4], refs[4:8], refs[8:]

    @pl.when(pl.program_id(0) == 0)
    def _():
        for p, o_ref in enumerate(o_refs):
            x_s[:, p * width:(p + 1) * width] = o_ref[0]

    for p, w_ref in enumerate(w_refs):
        w_s[p * width:(p + 1) * width, :] = w_ref[...]
    out = jnp.dot(x_s[...], w_s[...], preferred_element_type=F32)
    for add_ref in reversed(add_refs):
        out = out + add_ref[...].astype(F32)
    out_ref[...] = out.astype(out_ref.dtype)


def mix_mm(pieces, half, weights, dtype, added=()):
    _, rows, width = pieces[0].shape
    d_model = weights[0].shape[1]
    bn = 512
    o_spec = pl.BlockSpec((1, rows, width), lambda j: (half, 0, 0))
    w_spec = pl.BlockSpec((width, bn), lambda j: (0, j))
    return pl.pallas_call(
        functools.partial(mix_mm_kernel, width),
        out_shape=jax.ShapeDtypeStruct((rows, d_model), dtype),
        grid=(d_model // bn,),
        in_specs=[o_spec] * 4 + [w_spec] * 4 + [pl.BlockSpec((rows, bn), lambda j: (0, j))] * len(added),
        out_specs=pl.BlockSpec((rows, bn), lambda j: (0, j)),
        scratch_shapes=[pltpu.VMEM((rows, 4 * width), BF16), pltpu.VMEM((4 * width, bn), BF16)],
        compiler_params=pltpu.CompilerParams(dimension_semantics=("arbitrary",), vmem_limit_bytes=VMEM_LIMIT),
        cost_estimate=pl.CostEstimate(flops=2 * rows * 4 * width * d_model, bytes_accessed=2 * (4 * width + 2 * rows) * d_model, transcendentals=0),
        name="mix_mm",
    )(*pieces, *weights, *added)


def finish_kernel(part, own_ref, got_ref, x_ref, dy_ref, gain_ref, *refs):
    dx_ref, dg_ref = refs[-2:]
    x = x_ref[...].astype(F32)
    inv_rms = lax.rsqrt(jnp.mean(x * x, axis=-1, keepdims=True) + NORM_EPS)
    x_hat = x * inv_rms
    d_hidden = (own_ref[...] + got_ref[...].astype(F32)).astype(BF16).astype(F32)

    @pl.when(pl.program_id(0) == 0)
    def _():
        dg_ref[...] = refs[1][...] if part else jnp.zeros_like(dg_ref)

    dg_ref[...] += jnp.sum(d_hidden * x_hat, axis=0, keepdims=True)
    scaled = d_hidden * gain_ref[...]
    d_input = inv_rms * (scaled - x_hat * jnp.mean(scaled * x_hat, axis=-1, keepdims=True))
    dx_ref[...] = (dy_ref[...].astype(F32) + d_input).astype(BF16)


def finish(part, parts, carry, dh_own, dh_got, x_blk, dy_blk, norm_gain):
    rows, d_model = x_blk.shape
    blk_rows = 64
    steps = rows // parts // blk_rows
    blk = pl.BlockSpec((blk_rows, d_model), lambda i: (i + part * steps, 0))
    got = pl.BlockSpec((blk_rows, d_model), lambda i: (i, 0))
    one = pl.BlockSpec((1, d_model), lambda i: (0, 0))
    operands = [dh_own, dh_got, x_blk, dy_blk, norm_gain[None, :]]
    in_specs = [blk, got, blk, blk, one]
    aliases = {}
    if part:
        aliases = {5: 0}
        operands += list(carry)
        in_specs += [pl.BlockSpec(memory_space=pl.ANY), one]
    return pl.pallas_call(
        functools.partial(finish_kernel, part),
        out_shape=(jax.ShapeDtypeStruct((rows, d_model), BF16), jax.ShapeDtypeStruct((1, d_model), F32)),
        grid=(steps,),
        in_specs=in_specs,
        out_specs=[blk, one],
        input_output_aliases=aliases,
        compiler_params=pltpu.CompilerParams(dimension_semantics=("arbitrary",), vmem_limit_bytes=VMEM_LIMIT),
        cost_estimate=pl.CostEstimate(flops=20 * rows * d_model // parts, bytes_accessed=12 * rows * d_model // parts, transcendentals=0),
    )(*operands)


def swap(value, bit, tp_size):
    return lax.ppermute(value, 'tp', [(d, d ^ bit) for d in range(tp_size)])


def pack_kernel(n_in, owner_ref, *refs):
    ins, outs = refs[:4 * n_in], refs[4 * n_in:]
    for p, out_ref in enumerate(outs):
        at = 0
        for ref in ins[p * n_in:(p + 1) * n_in]:
            out_ref[0, :, at:at + ref.shape[2]] = ref[0]
            at += ref.shape[2]


def group_rows(blocks, me, pair_bit, mate_bit, tp_size):
    bits = (0, 1, pair_bit, pair_bit | 1)
    owners = jnp.stack([me ^ bit ^ mate for bit in bits for mate in (0, mate_bit)])
    rows = blocks[0].shape[1]
    span = sum(b.shape[2] for b in blocks)
    in_specs = [pl.BlockSpec((1, rows, b.shape[2]), functools.partial(lambda p, h, owner: (owner[2 * p + h], 0, 0), p)) for p in range(4) for b in blocks]
    sent = pl.pallas_call(
        functools.partial(pack_kernel, len(blocks)),
        out_shape=[jax.ShapeDtypeStruct((2, rows, span), BF16)] * 4,
        grid_spec=pltpu.PrefetchScalarGridSpec(num_scalar_prefetch=1, grid=(2,), in_specs=in_specs,
                                               out_specs=[pl.BlockSpec((1, rows, span), lambda h, owner: (h, 0, 0))] * 4),
        compiler_params=pltpu.CompilerParams(dimension_semantics=("arbitrary",), vmem_limit_bytes=VMEM_LIMIT),
        cost_estimate=pl.CostEstimate(flops=0, bytes_accessed=32 * rows * span, transcendentals=0),
        name="pack_rows",
    )(owners, *(list(blocks) * 4))
    pieces = [sent[0]]
    for bit, rows_sent in zip(bits[1:], sent[1:]):
        pieces.append(swap(rows_sent, bit, tp_size))
    return pieces


def solution(mesh):
    tp_size = mesh.shape['tp']
    x_bit, y_bit = 2, 4

    def layer(x_blk, dy_blk, positions, norm_gain, wq_loc, wk_all, wv_all, wo_loc):
        heads = wq_loc.shape[1] // HEAD_DIM
        width = heads * HEAD_DIM
        rows, _ = x_blk.shape
        me = lax.axis_index('tp')

        def head_of(weights, owner):
            return lax.dynamic_slice_in_dim(weights, owner * HEAD_DIM, HEAD_DIM, axis=1)

        wqkv = jnp.concatenate([wq_loc, head_of(wk_all, me), head_of(wv_all, me)], axis=1)

        x_f32 = x_blk.astype(F32)
        hidden = norm_forward(x_f32, norm_gain)
        h_full = lax.all_gather(hidden, 'tp', axis=0, tiled=True)
        seq = h_full.shape[0]
        parts = rows // BQ
        dy_late, _ = lax.optimization_barrier((dy_blk, hidden))
        dy_in = [dy_late[p * BQ:(p + 1) * BQ] for p in range(parts)]
        dy_full = [lax.all_gather(dy_in[0], 'tp', axis=0, tiled=True)]

        cos_t, sin_t = rope_tables(positions)
        doc_start = lax.iota(jnp.int32, seq) - positions
        lo = doc_start[::BQ] // BK
        full = (doc_start[BQ - 1::BQ] + BK - 1) // BK

        h_full, cos_t, sin_t, lo, full, doc_start, wqkv = lax.optimization_barrier((h_full, cos_t, sin_t, lo, full, doc_start, wqkv))
        qkv = dot32(h_full, wqkv).astype(BF16)
        *dy_rest, qkv = lax.optimization_barrier((*dy_in[1:], qkv))
        dy_full += [lax.all_gather(dy_part, 'tp', axis=0, tiled=True) for dy_part in dy_rest]
        o, lse = attend_forward(lo, full, qkv, cos_t, sin_t, doc_start, heads)
        dy_full[0], o = lax.optimization_barrier((dy_full[0], o))
        o_blocks = o.reshape(tp_size, parts, BQ, width)
        carry = None
        for p in range(parts - 1):
            d_o = dot32(dy_full[p], wo_loc, NT).astype(BF16)
            carry = attend_backward(p, parts, carry, lo, full, qkv, o, d_o, lse, cos_t, sin_t, doc_start, heads)
        dy_full[-1], o_sent, wo_own, wq_own = lax.optimization_barrier((dy_full[-1], o, wo_loc, wq_loc))
        wq_near = swap(wq_own, y_bit, tp_size)
        wo_near = swap(wo_own, x_bit, tp_size)
        o_pieces = group_rows([o_sent.reshape(tp_size, rows, width)], me, x_bit, y_bit, tp_size)

        d_o = dot32(dy_full[-1], wo_loc, NT).astype(BF16)
        d_q, d_kv = attend_backward(parts - 1, parts, carry, lo, full, qkv, o, d_o, lse, cos_t, sin_t, doc_start, heads)
        dq_pieces = group_rows([d_q.reshape(tp_size, rows, width), d_kv.reshape(tp_size, rows, 2 * HEAD_DIM)], me, y_bit, x_bit, tp_size)
        d_wq = dot32(h_full, d_q, TN).astype(BF16)
        d_wkv = dot32(h_full, d_kv, TN)
        wq_near, wq_own, d_wq, d_wkv = lax.optimization_barrier((wq_near, wq_own, d_wq, d_wkv))
        wq_side = swap(wq_own, 1, tp_size)
        wq_group = [wq_own, wq_side, wq_near, swap(wq_near, 1, tp_size)]
        wo_near, wo_own, d_wkv = lax.optimization_barrier((wo_near, wo_own, d_wkv))
        wo_side = swap(wo_own, 1, tp_size)
        wo_group = [wo_own, wo_side, wo_near, swap(wo_near, 1, tp_size)]
        o_blocks, d_wkv = lax.optimization_barrier((o_blocks, d_wkv))
        d_wo = dot32(o_blocks[:, 0].reshape(-1, width), dy_full[0], TN)
        d_wo = (d_wo + sum(dot32(o_blocks[:, p].reshape(-1, width), dy_full[p], TN) for p in range(1, parts))).astype(BF16)
        mix_mate = mix_mm(o_pieces, 1, wo_group, BF16)
        dq_pieces, mix_mate, d_wq, d_wkv = lax.optimization_barrier((dq_pieces, mix_mate, d_wq, d_wkv))
        mix_got = swap(mix_mate, y_bit, tp_size)
        owners = jnp.stack([me ^ bit for bit in (0, 1, y_bit, y_bit | 1)])
        halves = 2
        dh_mate = grad_mm(owners, dq_pieces, 1, wq_group, wk_all, wv_all, BF16, halves)
        dh_got = []
        for p in range(halves):
            dh_got.append(swap(dh_mate[p], x_bit, tp_size))
        dh_own, = grad_mm(owners, dq_pieces, 0, wq_group, wk_all, wv_all, F32)
        mix_got, dh_own = lax.optimization_barrier((mix_got, dh_own))
        result = mix_mm(o_pieces, 0, wo_group, BF16, (x_blk, mix_got))
        d_wk, d_wv = d_wkv[:, :HEAD_DIM], d_wkv[:, HEAD_DIM:]
        dh_own, dh_got[0], result, d_wo, d_wk, d_wv = lax.optimization_barrier((dh_own, dh_got[0], result, d_wo, d_wk, d_wv))
        done = None
        for p in range(halves):
            done = finish(p, halves, done, dh_own, dh_got[p], x_blk, dy_blk, norm_gain)
        grad_x, d_gain = done[0], sum_over_tp(done[1][0], tp_size)
        return result, grad_x, d_wq, d_wk, d_wv, d_wo, d_gain

    specs_in = (P(('dp', 'tp'), None), P(('dp', 'tp'), None), P('dp'), P(), P(None, 'tp'), P(), P(), P('tp', None))
    specs_out = (P(('dp', 'tp'), None), P(('dp', 'tp'), None), P('dp', 'tp'), P('dp', 'tp'), P('dp', 'tp'), P(('dp', 'tp'), None), P('dp'))
    return jax.shard_map(layer, mesh=mesh, in_specs=specs_in, out_specs=specs_out, check_vma=False)
```

```python
import functools
import jax
import jax.numpy as jnp
from jax import lax
from jax.experimental import pallas as pl
from jax.experimental.pallas import tpu as pltpu
from jax.sharding import PartitionSpec as P

HEAD_DIM = 128
SCORE_SCALE = HEAD_DIM ** -0.5
LOG2_SCALE = SCORE_SCALE * 1.4426950408889634
ROPE_THETA = 1000000.0
NORM_EPS = 1e-05
MASKED = -1e30
BQ = 256
BK = 512
BK_BWD = 256
VMEM_LIMIT = 60 * 1024 * 1024
NT = (((1,), (1,)), ((), ()))
TN = (((0,), (0,)), ((), ()))
F32 = jnp.float32
BF16 = jnp.bfloat16


def rope_tables(positions):
    exponents = jnp.arange(0, HEAD_DIM, 2, dtype=F32) / HEAD_DIM
    angles = positions.astype(F32)[..., None] * jnp.power(ROPE_THETA, -exponents)
    cos_t, sin_t = jnp.cos(angles), jnp.sin(angles)
    return jnp.concatenate([cos_t, cos_t], axis=-1), jnp.concatenate([-sin_t, sin_t], axis=-1)


def rope(x, cos_t, sin_t):
    x = x.astype(F32)
    return (x * cos_t + pltpu.roll(x, HEAD_DIM // 2, 1) * sin_t).astype(BF16)


def rope_back(x, cos_t, sin_t):
    x = x.astype(F32)
    return (x * cos_t - pltpu.roll(x, HEAD_DIM // 2, 1) * sin_t).astype(BF16)


def stack_heads(x, heads):
    return jnp.concatenate([x[:, h * HEAD_DIM:(h + 1) * HEAD_DIM] for h in range(heads)], axis=0)


def key_loops(i, lo_ref, full_ref, bq, bk, body):
    first = lo_ref[i]
    below = (i * bq) // bk
    last = ((i + 1) * bq + bk - 1) // bk
    mid = jnp.minimum(jnp.maximum(full_ref[i], first), last)
    mid_end = jnp.maximum(mid, jnp.minimum(below, last))
    lax.fori_loop(first, mid, functools.partial(body, True), None)
    lax.fori_loop(mid, mid_end, functools.partial(body, False), None)
    lax.fori_loop(mid_end, last, functools.partial(body, True), None)


def fwd_kernel(heads, lo_ref, full_ref, q_ref, k_ref, v_ref, cos_ref, sin_ref, cosf_ref, sinf_ref, ds_ref, o_ref, lse_ref, k_s, m_s, l_s, acc_s):
    i = pl.program_id(0)
    bq, bk = BQ, BK

    @pl.when(i == 0)
    def _():
        k_s[...] = rope(k_ref[...], cosf_ref[...], sinf_ref[...])

    cos_t, sin_t = cos_ref[...], sin_ref[...]
    q4 = jnp.concatenate([rope(q_ref[:, h * HEAD_DIM:(h + 1) * HEAD_DIM], cos_t, sin_t) for h in range(heads)], axis=0)
    m_s[...] = jnp.full_like(m_s, MASKED)
    l_s[...] = jnp.zeros_like(l_s)
    acc_s[...] = jnp.zeros_like(acc_s)

    def body(masked, j, _):
        start = pl.multiple_of(j * bk, bk)
        kj = k_s[pl.ds(start, bk), :]
        vj = v_ref[pl.ds(start, bk), :]
        s = lax.dot_general(q4, kj, NT, preferred_element_type=F32) * LOG2_SCALE
        if masked:
            q_idx = i * bq + lax.broadcasted_iota(jnp.int32, (bq, bk), 0)
            k_idx = start + lax.broadcasted_iota(jnp.int32, (bq, bk), 1)
            keep = (k_idx <= q_idx) & (k_idx >= ds_ref[...])
            s = jnp.concatenate([jnp.where(keep, s[h * bq:(h + 1) * bq], MASKED) for h in range(heads)], axis=0)
        m_prev = m_s[...]
        m_new = jnp.maximum(m_prev, jnp.max(s, axis=1, keepdims=True))
        p = jnp.exp2(s - jnp.tile(m_new, (1, bk // HEAD_DIM)))
        alpha = jnp.exp2(m_prev - m_new)
        l_s[...] = l_s[...] * alpha + jnp.sum(p, axis=1, keepdims=True)
        m_s[...] = m_new
        acc_s[...] = acc_s[...] * alpha + jnp.dot(p.astype(BF16), vj, preferred_element_type=F32)

    key_loops(i, lo_ref, full_ref, bq, bk, body)
    l_all = l_s[...]
    o4 = (acc_s[...] / l_all).astype(BF16)
    for h in range(heads):
        o_ref[:, h * HEAD_DIM:(h + 1) * HEAD_DIM] = o4[h * bq:(h + 1) * bq]
    lse = m_s[...] + jnp.log2(l_all)
    lse_ref[0] = lse.T[0:1, :]


def bwd_kernel(heads, half, parts, n_blk, lo_ref, full_ref, q_ref, k_ref, v_ref, o_ref, do_ref, lse_ref, cos_ref, sin_ref, cosf_ref, sinf_ref, ds_ref, *refs):
    first, last = half == 0, half == parts - 1
    if not first:
        refs = refs[1:]
        dk_in, dv_in = refs[:2]
        refs = refs[2:]
    if last:
        dq_ref, dkv_ref, k_s, dq_s, dk_s, dv_s = refs
    else:
        dq_ref, dk_s, dv_s, k_s, dq_s = refs
    step = pl.program_id(0)
    i = step * parts + half
    bq, bk = BQ, BK_BWD

    @pl.when(step == 0)
    def _():
        k_s[...] = rope(k_ref[...], cosf_ref[...], sinf_ref[...])
        dk_s[...] = jnp.zeros_like(dk_s) if first else dk_in[...]
        dv_s[...] = jnp.zeros_like(dv_s) if first else dv_in[...]

    cos_t, sin_t = cos_ref[...], sin_ref[...]
    q4 = jnp.concatenate([rope(q_ref[:, h * HEAD_DIM:(h + 1) * HEAD_DIM], cos_t, sin_t) for h in range(heads)], axis=0)
    do4 = stack_heads(do_ref[...], heads)
    o4 = stack_heads(o_ref[...], heads)
    delta = jnp.sum((do4.astype(F32) * o4.astype(F32)).T, axis=0, keepdims=True)
    lse = lse_ref[0]
    dq_s[...] = jnp.zeros_like(dq_s)

    def body(masked, j, _):
        start = pl.multiple_of(j * bk, bk)
        kj = k_s[pl.ds(start, bk), :]
        vj = v_ref[pl.ds(start, bk), :]
        s = lax.dot_general(kj, q4, NT, preferred_element_type=F32) * LOG2_SCALE
        if masked:
            q_idx = i * bq + lax.broadcasted_iota(jnp.int32, (bk, bq), 1)
            k_idx = start + lax.broadcasted_iota(jnp.int32, (bk, bq), 0)
            keep = (k_idx <= q_idx) & (k_idx >= ds_ref[0])
            s = jnp.concatenate([jnp.where(keep, s[:, h * bq:(h + 1) * bq], MASKED) for h in range(heads)], axis=1)
        p = jnp.exp2(s - lse)
        dp = lax.dot_general(vj, do4, NT, preferred_element_type=F32)
        dv_s[pl.ds(start, bk), :] += jnp.dot(p.astype(BF16), do4, preferred_element_type=F32)
        d_s = (p * (dp - delta)).astype(BF16)
        dk_s[pl.ds(start, bk), :] += jnp.dot(d_s, q4, preferred_element_type=F32)
        dq_s[...] += lax.dot_general(d_s, kj, TN, preferred_element_type=F32)

    key_loops(i, lo_ref, full_ref, bq, bk, body)
    for h in range(heads):
        dq = (dq_s[h * bq:(h + 1) * bq, :] * SCORE_SCALE).astype(BF16)
        dq_ref[:, h * HEAD_DIM:(h + 1) * HEAD_DIM] = rope_back(dq, cos_t, sin_t)

    if last:
        @pl.when(step == n_blk - 1)
        def _():
            dk = (dk_s[...] * SCORE_SCALE).astype(BF16)
            dkv_ref[:, :HEAD_DIM] = rope_back(dk, cosf_ref[...], sinf_ref[...])
            dkv_ref[:, HEAD_DIM:] = dv_s[...].astype(BF16)


def attention_specs(seq, heads):
    width = heads * HEAD_DIM
    q_spec = pl.BlockSpec((BQ, width), lambda i, *_: (i, 0))
    k_spec = pl.BlockSpec((seq, HEAD_DIM), lambda i, *_: (0, heads))
    v_spec = pl.BlockSpec((seq, HEAD_DIM), lambda i, *_: (0, heads + 1))
    tab_spec = pl.BlockSpec((BQ, HEAD_DIM), lambda i, *_: (i, 0))
    tabf_spec = pl.BlockSpec((seq, HEAD_DIM), lambda i, *_: (0, 0))
    row_spec = pl.BlockSpec((1, 1, heads * BQ), lambda i, *_: (i, 0, 0))
    return q_spec, k_spec, v_spec, tab_spec, tabf_spec, row_spec


def attend_forward(lo, full, qkv, cos_t, sin_t, doc_start, heads):
    seq = qkv.shape[0]
    n_blk = seq // BQ
    q_spec, k_spec, v_spec, tab_spec, tabf_spec, row_spec = attention_specs(seq, heads)
    return pl.pallas_call(
        functools.partial(fwd_kernel, heads),
        out_shape=(jax.ShapeDtypeStruct((seq, heads * HEAD_DIM), BF16), jax.ShapeDtypeStruct((n_blk, 1, heads * BQ), F32)),
        grid_spec=pltpu.PrefetchScalarGridSpec(
            num_scalar_prefetch=2, grid=(n_blk,),
            in_specs=[q_spec, k_spec, v_spec, tab_spec, tab_spec, tabf_spec, tabf_spec, pl.BlockSpec((BQ, 1), lambda i, *_: (i, 0))],
            out_specs=[q_spec, row_spec],
            scratch_shapes=[pltpu.VMEM((seq, HEAD_DIM), BF16)] + [pltpu.VMEM((heads * BQ, HEAD_DIM), F32)] * 3),
        compiler_params=pltpu.CompilerParams(dimension_semantics=("arbitrary",), vmem_limit_bytes=VMEM_LIMIT),
        cost_estimate=pl.CostEstimate(flops=4 * heads * seq * seq // 2 * HEAD_DIM, bytes_accessed=16 * 2 ** 20, transcendentals=heads * seq * seq // 2),
        name="attend_fwd",
    )(lo, full, qkv, qkv, qkv, cos_t, sin_t, cos_t, sin_t, doc_start[:, None])


def attend_backward(half, parts, carry, lo, full, qkv, o, d_o, lse, cos_t, sin_t, doc_start, heads):
    seq = qkv.shape[0]
    n_blk = seq // BQ // parts
    width = heads * HEAD_DIM
    _, k_spec, v_spec, _, full_spec, _ = attention_specs(seq, heads)
    q_spec = pl.BlockSpec((BQ, width), lambda i, *_: (i * parts + half, 0))
    do_spec = pl.BlockSpec((BQ, width), lambda i, *_: (i, 0))
    tab_spec = pl.BlockSpec((BQ, HEAD_DIM), lambda i, *_: (i * parts + half, 0))
    row_spec = pl.BlockSpec((1, 1, heads * BQ), lambda i, *_: (i * parts + half, 0, 0))
    ds_spec = pl.BlockSpec((1, 1, BQ), lambda i, *_: (i * parts + half, 0, 0))
    in_specs = [q_spec, k_spec, v_spec, q_spec, do_spec, row_spec, tab_spec, tab_spec, full_spec, full_spec, ds_spec]
    operands = [lo, full, qkv, qkv, qkv, o, d_o, lse, cos_t, sin_t, cos_t, sin_t, doc_start.reshape(seq // BQ, 1, BQ)]
    aliases = {}
    if half:
        aliases = {len(operands): 0}
        in_specs += [pl.BlockSpec(memory_space=pl.ANY), full_spec, full_spec]
        operands += list(carry)
    dq_shape = jax.ShapeDtypeStruct((seq, width), BF16)
    sum_shape = jax.ShapeDtypeStruct((seq, HEAD_DIM), F32)
    scratch = [pltpu.VMEM((seq, HEAD_DIM), BF16), pltpu.VMEM((heads * BQ, HEAD_DIM), F32)]
    if half == parts - 1:
        out_shape = (dq_shape, jax.ShapeDtypeStruct((seq, 2 * HEAD_DIM), BF16))
        out_specs = [q_spec, pl.BlockSpec((seq, 2 * HEAD_DIM), lambda i, *_: (0, 0))]
        scratch += [pltpu.VMEM((seq, HEAD_DIM), F32)] * 2
    else:
        out_shape = (dq_shape, sum_shape, sum_shape)
        out_specs = [q_spec, full_spec, full_spec]
    return pl.pallas_call(
        functools.partial(bwd_kernel, heads, half, parts, n_blk),
        out_shape=out_shape,
        grid_spec=pltpu.PrefetchScalarGridSpec(num_scalar_prefetch=2, grid=(n_blk,), in_specs=in_specs, out_specs=out_specs, scratch_shapes=scratch),
        input_output_aliases=aliases,
        compiler_params=pltpu.CompilerParams(dimension_semantics=("arbitrary",), vmem_limit_bytes=VMEM_LIMIT),
        cost_estimate=pl.CostEstimate(flops=10 * heads * seq * seq // 2 * HEAD_DIM // parts, bytes_accessed=24 * 2 ** 20 // parts, transcendentals=heads * seq * seq // 2 // parts),
    )(*operands)


def norm_forward(x_f32, norm_gain):
    inv_rms = lax.rsqrt(jnp.mean(x_f32 * x_f32, axis=-1, keepdims=True) + NORM_EPS)
    return (x_f32 * inv_rms * norm_gain).astype(BF16)


def dot32(a, b, dims=(((1,), (0,)), ((), ()))):
    return lax.dot_general(a, b, dims, preferred_element_type=F32)


def sum_over_tp(value, tp_size):
    step = 1
    while step < tp_size:
        value = value + lax.ppermute(value, 'tp', [(d, d ^ step) for d in range(tp_size)])
        step *= 2
    return value


def grad_mm_kernel(width, owner_ref, *refs):
    g_refs, w_refs, (wk_ref, wv_ref, *out_refs, x_s, w_s) = refs[:4], refs[4:8], refs[8:]
    span = width + 2 * HEAD_DIM

    @pl.when(pl.program_id(0) == 0)
    def _():
        for p, g_ref in enumerate(g_refs):
            x_s[:, p * span:(p + 1) * span] = g_ref[0]

    for p, w_ref in enumerate(w_refs):
        head = pl.ds(pl.multiple_of(owner_ref[p] * HEAD_DIM, HEAD_DIM), HEAD_DIM)
        w_s[:, p * span:p * span + width] = w_ref[...]
        w_s[:, p * span + width:p * span + width + HEAD_DIM] = wk_ref[:, head]
        w_s[:, p * span + width + HEAD_DIM:(p + 1) * span] = wv_ref[:, head]
    out = lax.dot_general(x_s[...], w_s[...], NT, preferred_element_type=F32)
    rows = out_refs[0].shape[0]
    for r, out_ref in enumerate(out_refs):
        out_ref[...] = out[r * rows:(r + 1) * rows].astype(out_ref.dtype)


def grad_mm(owners, pieces, half, weights, wk_all, wv_all, dtype, parts=1):
    _, rows, span = pieces[0].shape
    d_model, width = weights[0].shape
    bn = 512
    g_spec = pl.BlockSpec((1, rows, span), lambda j, *_: (half, 0, 0))
    w_spec = pl.BlockSpec((bn, width), lambda j, *_: (j, 0))
    kv_spec = pl.BlockSpec((bn, wk_all.shape[1]), lambda j, *_: (j, 0))
    return pl.pallas_call(
        functools.partial(grad_mm_kernel, width),
        out_shape=[jax.ShapeDtypeStruct((rows // parts, d_model), dtype)] * parts,
        grid_spec=pltpu.PrefetchScalarGridSpec(
            num_scalar_prefetch=1, grid=(d_model // bn,),
            in_specs=[g_spec] * 4 + [w_spec] * 4 + [kv_spec] * 2,
            out_specs=[pl.BlockSpec((rows // parts, bn), lambda j, *_: (0, j))] * parts,
            scratch_shapes=[pltpu.VMEM((rows, 4 * span), BF16), pltpu.VMEM((bn, 4 * span), BF16)]),
        compiler_params=pltpu.CompilerParams(dimension_semantics=("arbitrary",), vmem_limit_bytes=VMEM_LIMIT),
        cost_estimate=pl.CostEstimate(flops=2 * rows * 4 * span * d_model, bytes_accessed=2 * (4 * span + 2 * rows) * d_model, transcendentals=0),
        name="grad_mm",
    )(owners, *pieces, *weights, wk_all, wv_all)


def mix_mm_kernel(width, *refs):
    o_refs, w_refs, (*add_refs, out_ref, x_s, w_s) = refs[:4], refs[4:8], refs[8:]

    @pl.when(pl.program_id(0) == 0)
    def _():
        for p, o_ref in enumerate(o_refs):
            x_s[:, p * width:(p + 1) * width] = o_ref[0]

    for p, w_ref in enumerate(w_refs):
        w_s[p * width:(p + 1) * width, :] = w_ref[...]
    out = jnp.dot(x_s[...], w_s[...], preferred_element_type=F32)
    for add_ref in reversed(add_refs):
        out = out + add_ref[...].astype(F32)
    out_ref[...] = out.astype(out_ref.dtype)


def mix_mm(pieces, half, weights, dtype, added=()):
    _, rows, width = pieces[0].shape
    d_model = weights[0].shape[1]
    bn = 512
    o_spec = pl.BlockSpec((1, rows, width), lambda j: (half, 0, 0))
    w_spec = pl.BlockSpec((width, bn), lambda j: (0, j))
    return pl.pallas_call(
        functools.partial(mix_mm_kernel, width),
        out_shape=jax.ShapeDtypeStruct((rows, d_model), dtype),
        grid=(d_model // bn,),
        in_specs=[o_spec] * 4 + [w_spec] * 4 + [pl.BlockSpec((rows, bn), lambda j: (0, j))] * len(added),
        out_specs=pl.BlockSpec((rows, bn), lambda j: (0, j)),
        scratch_shapes=[pltpu.VMEM((rows, 4 * width), BF16), pltpu.VMEM((4 * width, bn), BF16)],
        compiler_params=pltpu.CompilerParams(dimension_semantics=("arbitrary",), vmem_limit_bytes=VMEM_LIMIT),
        cost_estimate=pl.CostEstimate(flops=2 * rows * 4 * width * d_model, bytes_accessed=2 * (4 * width + 2 * rows) * d_model, transcendentals=0),
        name="mix_mm",
    )(*pieces, *weights, *added)


def finish_kernel(part, own_ref, got_ref, x_ref, dy_ref, gain_ref, *refs):
    dx_ref, dg_ref = refs[-2:]
    x = x_ref[...].astype(F32)
    inv_rms = lax.rsqrt(jnp.mean(x * x, axis=-1, keepdims=True) + NORM_EPS)
    x_hat = x * inv_rms
    d_hidden = (own_ref[...] + got_ref[...].astype(F32)).astype(BF16).astype(F32)

    @pl.when(pl.program_id(0) == 0)
    def _():
        dg_ref[...] = refs[1][...] if part else jnp.zeros_like(dg_ref)

    dg_ref[...] += jnp.sum(d_hidden * x_hat, axis=0, keepdims=True)
    scaled = d_hidden * gain_ref[...]
    d_input = inv_rms * (scaled - x_hat * jnp.mean(scaled * x_hat, axis=-1, keepdims=True))
    dx_ref[...] = (dy_ref[...].astype(F32) + d_input).astype(BF16)


def finish(part, parts, carry, dh_own, dh_got, x_blk, dy_blk, norm_gain):
    rows, d_model = x_blk.shape
    blk_rows = 64
    steps = rows // parts // blk_rows
    blk = pl.BlockSpec((blk_rows, d_model), lambda i: (i + part * steps, 0))
    got = pl.BlockSpec((blk_rows, d_model), lambda i: (i, 0))
    one = pl.BlockSpec((1, d_model), lambda i: (0, 0))
    operands = [dh_own, dh_got, x_blk, dy_blk, norm_gain[None, :]]
    in_specs = [blk, got, blk, blk, one]
    aliases = {}
    if part:
        aliases = {5: 0}
        operands += list(carry)
        in_specs += [pl.BlockSpec(memory_space=pl.ANY), one]
    return pl.pallas_call(
        functools.partial(finish_kernel, part),
        out_shape=(jax.ShapeDtypeStruct((rows, d_model), BF16), jax.ShapeDtypeStruct((1, d_model), F32)),
        grid=(steps,),
        in_specs=in_specs,
        out_specs=[blk, one],
        input_output_aliases=aliases,
        compiler_params=pltpu.CompilerParams(dimension_semantics=("arbitrary",), vmem_limit_bytes=VMEM_LIMIT),
        cost_estimate=pl.CostEstimate(flops=20 * rows * d_model // parts, bytes_accessed=12 * rows * d_model // parts, transcendentals=0),
    )(*operands)


def swap(value, bit, tp_size):
    return lax.ppermute(value, 'tp', [(d, d ^ bit) for d in range(tp_size)])


def pack_kernel(n_in, owner_ref, *refs):
    ins, outs = refs[:4 * n_in], refs[4 * n_in:]
    for p, out_ref in enumerate(outs):
        at = 0
        for ref in ins[p * n_in:(p + 1) * n_in]:
            out_ref[0, :, at:at + ref.shape[2]] = ref[0]
            at += ref.shape[2]


def group_rows(blocks, me, pair_bit, mate_bit, tp_size):
    bits = (0, 1, pair_bit, pair_bit | 1)
    owners = jnp.stack([me ^ bit ^ mate for bit in bits for mate in (0, mate_bit)])
    rows = blocks[0].shape[1]
    span = sum(b.shape[2] for b in blocks)
    in_specs = [pl.BlockSpec((1, rows, b.shape[2]), functools.partial(lambda p, h, owner: (owner[2 * p + h], 0, 0), p)) for p in range(4) for b in blocks]
    sent = pl.pallas_call(
        functools.partial(pack_kernel, len(blocks)),
        out_shape=[jax.ShapeDtypeStruct((2, rows, span), BF16)] * 4,
        grid_spec=pltpu.PrefetchScalarGridSpec(num_scalar_prefetch=1, grid=(2,), in_specs=in_specs,
                                               out_specs=[pl.BlockSpec((1, rows, span), lambda h, owner: (h, 0, 0))] * 4),
        compiler_params=pltpu.CompilerParams(dimension_semantics=("arbitrary",), vmem_limit_bytes=VMEM_LIMIT),
        cost_estimate=pl.CostEstimate(flops=0, bytes_accessed=32 * rows * span, transcendentals=0),
        name="pack_rows",
    )(owners, *(list(blocks) * 4))
    pieces = [sent[0]]
    for bit, rows_sent in zip(bits[1:], sent[1:]):
        pieces.append(swap(rows_sent, bit, tp_size))
    return pieces


def solution(mesh):
    tp_size = mesh.shape['tp']
    x_bit, y_bit = 2, 4

    def layer(x_blk, dy_blk, positions, norm_gain, wq_loc, wk_all, wv_all, wo_loc):
        heads = wq_loc.shape[1] // HEAD_DIM
        width = heads * HEAD_DIM
        rows, _ = x_blk.shape
        me = lax.axis_index('tp')

        def head_of(weights, owner):
            return lax.dynamic_slice_in_dim(weights, owner * HEAD_DIM, HEAD_DIM, axis=1)

        wqkv = jnp.concatenate([wq_loc, head_of(wk_all, me), head_of(wv_all, me)], axis=1)

        x_f32 = x_blk.astype(F32)
        hidden = norm_forward(x_f32, norm_gain)
        h_full = lax.all_gather(hidden, 'tp', axis=0, tiled=True)
        seq = h_full.shape[0]
        parts = rows // BQ
        dy_late, _ = lax.optimization_barrier((dy_blk, hidden))
        dy_in = [dy_late[p * BQ:(p + 1) * BQ] for p in range(parts)]
        dy_full = [lax.all_gather(dy_in[0], 'tp', axis=0, tiled=True)]

        cos_t, sin_t = rope_tables(positions)
        doc_start = lax.iota(jnp.int32, seq) - positions
        lo, lo_bwd = doc_start[::BQ] // BK, doc_start[::BQ] // BK_BWD
        full, full_bwd = (doc_start[BQ - 1::BQ] + BK - 1) // BK, (doc_start[BQ - 1::BQ] + BK_BWD - 1) // BK_BWD

        h_full, cos_t, sin_t, lo, full, doc_start, wqkv = lax.optimization_barrier((h_full, cos_t, sin_t, lo, full, doc_start, wqkv))
        qkv = dot32(h_full, wqkv).astype(BF16)
        *dy_rest, qkv = lax.optimization_barrier((*dy_in[1:], qkv))
        dy_full += [lax.all_gather(dy_part, 'tp', axis=0, tiled=True) for dy_part in dy_rest]
        o, lse = attend_forward(lo, full, qkv, cos_t, sin_t, doc_start, heads)
        dy_full[0], o = lax.optimization_barrier((dy_full[0], o))
        o_blocks = o.reshape(tp_size, parts, BQ, width)
        carry = None
        for p in range(parts - 1):
            d_o = dot32(dy_full[p], wo_loc, NT).astype(BF16)
            carry = attend_backward(p, parts, carry, lo_bwd, full_bwd, qkv, o, d_o, lse, cos_t, sin_t, doc_start, heads)
        dy_full[-1], o_sent, wo_own, wq_own = lax.optimization_barrier((dy_full[-1], o, wo_loc, wq_loc))
        wq_near = swap(wq_own, y_bit, tp_size)
        wo_near = swap(wo_own, x_bit, tp_size)
        o_pieces = group_rows([o_sent.reshape(tp_size, rows, width)], me, x_bit, y_bit, tp_size)

        d_o = dot32(dy_full[-1], wo_loc, NT).astype(BF16)
        d_q, d_kv = attend_backward(parts - 1, parts, carry, lo_bwd, full_bwd, qkv, o, d_o, lse, cos_t, sin_t, doc_start, heads)
        dq_pieces = group_rows([d_q.reshape(tp_size, rows, width), d_kv.reshape(tp_size, rows, 2 * HEAD_DIM)], me, y_bit, x_bit, tp_size)
        d_wq = dot32(h_full, d_q, TN).astype(BF16)
        d_wkv = dot32(h_full, d_kv, TN)
        wq_near, wq_own, d_wq, d_wkv = lax.optimization_barrier((wq_near, wq_own, d_wq, d_wkv))
        wq_side = swap(wq_own, 1, tp_size)
        wq_group = [wq_own, wq_side, wq_near, swap(wq_near, 1, tp_size)]
        wo_near, wo_own, d_wkv = lax.optimization_barrier((wo_near, wo_own, d_wkv))
        wo_side = swap(wo_own, 1, tp_size)
        wo_group = [wo_own, wo_side, wo_near, swap(wo_near, 1, tp_size)]
        o_blocks, d_wkv = lax.optimization_barrier((o_blocks, d_wkv))
        d_wo = dot32(o_blocks[:, 0].reshape(-1, width), dy_full[0], TN)
        mix_mate = mix_mm(o_pieces, 1, wo_group, BF16)
        dq_pieces, mix_mate, d_wq, d_wkv = lax.optimization_barrier((dq_pieces, mix_mate, d_wq, d_wkv))
        mix_got = swap(mix_mate, y_bit, tp_size)
        owners = jnp.stack([me ^ bit for bit in (0, 1, y_bit, y_bit | 1)])
        halves = 2
        dh_mate = list(grad_mm(owners, dq_pieces, 1, wq_group, wk_all, wv_all, BF16, halves))
        o_blocks, dh_mate[0] = lax.optimization_barrier((o_blocks, dh_mate[0]))
        for p in range(1, parts):
            d_wo = d_wo + dot32(o_blocks[:, p].reshape(-1, width), dy_full[p], TN)
        d_wo = d_wo.astype(BF16)
        dh_got = []
        for p in range(halves):
            dh_got.append(swap(dh_mate[p], x_bit, tp_size))
        dh_own, = grad_mm(owners, dq_pieces, 0, wq_group, wk_all, wv_all, F32)
        mix_got, dh_own = lax.optimization_barrier((mix_got, dh_own))
        result = mix_mm(o_pieces, 0, wo_group, BF16, (x_blk, mix_got))
        d_wk, d_wv = d_wkv[:, :HEAD_DIM], d_wkv[:, HEAD_DIM:]
        dh_own, dh_got[0], result, d_wo, d_wk, d_wv = lax.optimization_barrier((dh_own, dh_got[0], result, d_wo, d_wk, d_wv))
        done = None
        for p in range(halves):
            done = finish(p, halves, done, dh_own, dh_got[p], x_blk, dy_blk, norm_gain)
        grad_x, d_gain = done[0], sum_over_tp(done[1][0], tp_size)
        return result, grad_x, d_wq, d_wk, d_wv, d_wo, d_gain

    specs_in = (P(('dp', 'tp'), None), P(('dp', 'tp'), None), P('dp'), P(), P(None, 'tp'), P(), P(), P('tp', None))
    specs_out = (P(('dp', 'tp'), None), P(('dp', 'tp'), None), P('dp', 'tp'), P('dp', 'tp'), P('dp', 'tp'), P(('dp', 'tp'), None), P('dp'))
    return jax.shard_map(layer, mesh=mesh, in_specs=specs_in, out_specs=specs_out, check_vma=False)
```

```python
import functools
import jax
import jax.numpy as jnp
from jax import lax
from jax.experimental import pallas as pl
from jax.experimental.pallas import tpu as pltpu
from jax.sharding import PartitionSpec as P

HEAD_DIM = 128
SCORE_SCALE = HEAD_DIM ** -0.5
LOG2_SCALE = SCORE_SCALE * 1.4426950408889634
ROPE_THETA = 1000000.0
NORM_EPS = 1e-05
MASKED = -1e30
BQ = 256
BK = 512
BK_BWD = 256
VMEM_LIMIT = 60 * 1024 * 1024
NT = (((1,), (1,)), ((), ()))
TN = (((0,), (0,)), ((), ()))
F32 = jnp.float32
BF16 = jnp.bfloat16


def rope_tables(positions):
    exponents = jnp.arange(0, HEAD_DIM, 2, dtype=F32) / HEAD_DIM
    angles = positions.astype(F32)[..., None] * jnp.power(ROPE_THETA, -exponents)
    cos_t, sin_t = jnp.cos(angles), jnp.sin(angles)
    return jnp.concatenate([cos_t, cos_t], axis=-1), jnp.concatenate([-sin_t, sin_t], axis=-1)


def rope(x, cos_t, sin_t):
    x = x.astype(F32)
    return (x * cos_t + pltpu.roll(x, HEAD_DIM // 2, 1) * sin_t).astype(BF16)


def rope_back(x, cos_t, sin_t):
    x = x.astype(F32)
    return (x * cos_t - pltpu.roll(x, HEAD_DIM // 2, 1) * sin_t).astype(BF16)


def stack_heads(x, heads):
    return jnp.concatenate([x[:, h * HEAD_DIM:(h + 1) * HEAD_DIM] for h in range(heads)], axis=0)


def key_loops(i, lo_ref, full_ref, bq, bk, body):
    first = lo_ref[i]
    below = (i * bq) // bk
    last = ((i + 1) * bq + bk - 1) // bk
    mid = jnp.minimum(jnp.maximum(full_ref[i], first), last)
    mid_end = jnp.maximum(mid, jnp.minimum(below, last))
    lax.fori_loop(first, mid, functools.partial(body, True), None)
    lax.fori_loop(mid, mid_end, functools.partial(body, False), None)
    lax.fori_loop(mid_end, last, functools.partial(body, True), None)


def fwd_kernel(heads, lo_ref, full_ref, q_ref, k_ref, v_ref, cos_ref, sin_ref, cosf_ref, sinf_ref, ds_ref, o_ref, lse_ref, k_s, m_s, l_s, acc_s):
    i = pl.program_id(0)
    bq, bk = BQ, BK

    @pl.when(i == 0)
    def _():
        k_s[...] = rope(k_ref[...], cosf_ref[...], sinf_ref[...])

    cos_t, sin_t = cos_ref[...], sin_ref[...]
    q4 = jnp.concatenate([rope(q_ref[:, h * HEAD_DIM:(h + 1) * HEAD_DIM], cos_t, sin_t) for h in range(heads)], axis=0)
    m_s[...] = jnp.full_like(m_s, MASKED)
    l_s[...] = jnp.zeros_like(l_s)
    acc_s[...] = jnp.zeros_like(acc_s)

    def body(masked, j, _):
        start = pl.multiple_of(j * bk, bk)
        kj = k_s[pl.ds(start, bk), :]
        vj = v_ref[pl.ds(start, bk), :]
        s = lax.dot_general(q4, kj, NT, preferred_element_type=F32) * LOG2_SCALE
        if masked:
            q_idx = i * bq + lax.broadcasted_iota(jnp.int32, (bq, bk), 0)
            k_idx = start + lax.broadcasted_iota(jnp.int32, (bq, bk), 1)
            keep = (k_idx <= q_idx) & (k_idx >= ds_ref[...])
            s = jnp.concatenate([jnp.where(keep, s[h * bq:(h + 1) * bq], MASKED) for h in range(heads)], axis=0)
        m_prev = m_s[...]
        m_new = jnp.maximum(m_prev, jnp.max(s, axis=1, keepdims=True))
        p = jnp.exp2(s - jnp.tile(m_new, (1, bk // HEAD_DIM)))
        alpha = jnp.exp2(m_prev - m_new)
        l_s[...] = l_s[...] * alpha + jnp.sum(p, axis=1, keepdims=True)
        m_s[...] = m_new
        acc_s[...] = acc_s[...] * alpha + jnp.dot(p.astype(BF16), vj, preferred_element_type=F32)

    key_loops(i, lo_ref, full_ref, bq, bk, body)
    l_all = l_s[...]
    o4 = (acc_s[...] / l_all).astype(BF16)
    for h in range(heads):
        o_ref[:, h * HEAD_DIM:(h + 1) * HEAD_DIM] = o4[h * bq:(h + 1) * bq]
    lse = m_s[...] + jnp.log2(l_all)
    lse_ref[0] = lse.T[0:1, :]


def bwd_kernel(heads, half, parts, n_blk, lo_ref, full_ref, q_ref, k_ref, v_ref, o_ref, do_ref, lse_ref, cos_ref, sin_ref, cosf_ref, sinf_ref, ds_ref, *refs):
    first, last = half == 0, half == parts - 1
    if not first:
        refs = refs[1:]
        dk_in, dv_in = refs[:2]
        refs = refs[2:]
    if last:
        dq_ref, dkv_ref, k_s, dq_s, dk_s, dv_s = refs
    else:
        dq_ref, dk_s, dv_s, k_s, dq_s = refs
    step = pl.program_id(0)
    i = step * parts + half
    bq, bk = BQ, BK_BWD

    @pl.when(step == 0)
    def _():
        k_s[...] = rope(k_ref[...], cosf_ref[...], sinf_ref[...])
        dk_s[...] = jnp.zeros_like(dk_s) if first else dk_in[...]
        dv_s[...] = jnp.zeros_like(dv_s) if first else dv_in[...]

    cos_t, sin_t = cos_ref[...], sin_ref[...]
    q4 = jnp.concatenate([rope(q_ref[:, h * HEAD_DIM:(h + 1) * HEAD_DIM], cos_t, sin_t) for h in range(heads)], axis=0)
    do4 = stack_heads(do_ref[...], heads)
    o4 = stack_heads(o_ref[...], heads)
    delta = jnp.sum((do4.astype(F32) * o4.astype(F32)).T, axis=0, keepdims=True)
    lse = lse_ref[0]
    dq_s[...] = jnp.zeros_like(dq_s)

    def body(masked, j, _):
        start = pl.multiple_of(j * bk, bk)
        kj = k_s[pl.ds(start, bk), :]
        vj = v_ref[pl.ds(start, bk), :]
        s = lax.dot_general(kj, q4, NT, preferred_element_type=F32) * LOG2_SCALE
        if masked:
            q_idx = i * bq + lax.broadcasted_iota(jnp.int32, (bk, bq), 1)
            k_idx = start + lax.broadcasted_iota(jnp.int32, (bk, bq), 0)
            keep = (k_idx <= q_idx) & (k_idx >= ds_ref[0])
            s = jnp.concatenate([jnp.where(keep, s[:, h * bq:(h + 1) * bq], MASKED) for h in range(heads)], axis=1)
        p = jnp.exp2(s - lse)
        dp = lax.dot_general(vj, do4, NT, preferred_element_type=F32)
        dv_s[pl.ds(start, bk), :] += jnp.dot(p.astype(BF16), do4, preferred_element_type=F32)
        d_s = (p * (dp - delta)).astype(BF16)
        dk_s[pl.ds(start, bk), :] += jnp.dot(d_s, q4, preferred_element_type=F32)
        dq_s[...] += lax.dot_general(d_s, kj, TN, preferred_element_type=F32)

    key_loops(i, lo_ref, full_ref, bq, bk, body)
    for h in range(heads):
        dq = (dq_s[h * bq:(h + 1) * bq, :] * SCORE_SCALE).astype(BF16)
        dq_ref[:, h * HEAD_DIM:(h + 1) * HEAD_DIM] = rope_back(dq, cos_t, sin_t)

    if last:
        @pl.when(step == n_blk - 1)
        def _():
            dk = (dk_s[...] * SCORE_SCALE).astype(BF16)
            dkv_ref[:, :HEAD_DIM] = rope_back(dk, cosf_ref[...], sinf_ref[...])
            dkv_ref[:, HEAD_DIM:] = dv_s[...].astype(BF16)


def attention_specs(seq, heads):
    width = heads * HEAD_DIM
    q_spec = pl.BlockSpec((BQ, width), lambda i, *_: (i, 0))
    k_spec = pl.BlockSpec((seq, HEAD_DIM), lambda i, *_: (0, heads))
    v_spec = pl.BlockSpec((seq, HEAD_DIM), lambda i, *_: (0, heads + 1))
    tab_spec = pl.BlockSpec((BQ, HEAD_DIM), lambda i, *_: (i, 0))
    tabf_spec = pl.BlockSpec((seq, HEAD_DIM), lambda i, *_: (0, 0))
    row_spec = pl.BlockSpec((1, 1, heads * BQ), lambda i, *_: (i, 0, 0))
    return q_spec, k_spec, v_spec, tab_spec, tabf_spec, row_spec


def attend_forward(lo, full, qkv, cos_t, sin_t, doc_start, heads):
    seq = qkv.shape[0]
    n_blk = seq // BQ
    q_spec, k_spec, v_spec, tab_spec, tabf_spec, row_spec = attention_specs(seq, heads)
    return pl.pallas_call(
        functools.partial(fwd_kernel, heads),
        out_shape=(jax.ShapeDtypeStruct((seq, heads * HEAD_DIM), BF16), jax.ShapeDtypeStruct((n_blk, 1, heads * BQ), F32)),
        grid_spec=pltpu.PrefetchScalarGridSpec(
            num_scalar_prefetch=2, grid=(n_blk,),
            in_specs=[q_spec, k_spec, v_spec, tab_spec, tab_spec, tabf_spec, tabf_spec, pl.BlockSpec((BQ, 1), lambda i, *_: (i, 0))],
            out_specs=[q_spec, row_spec],
            scratch_shapes=[pltpu.VMEM((seq, HEAD_DIM), BF16)] + [pltpu.VMEM((heads * BQ, HEAD_DIM), F32)] * 3),
        compiler_params=pltpu.CompilerParams(dimension_semantics=("arbitrary",), vmem_limit_bytes=VMEM_LIMIT),
        cost_estimate=pl.CostEstimate(flops=4 * heads * seq * seq // 2 * HEAD_DIM, bytes_accessed=16 * 2 ** 20, transcendentals=heads * seq * seq // 2),
        name="attend_fwd",
    )(lo, full, qkv, qkv, qkv, cos_t, sin_t, cos_t, sin_t, doc_start[:, None])


def attend_backward(half, parts, carry, lo, full, qkv, o, d_o, lse, cos_t, sin_t, doc_start, heads):
    seq = qkv.shape[0]
    n_blk = seq // BQ // parts
    width = heads * HEAD_DIM
    _, k_spec, v_spec, _, full_spec, _ = attention_specs(seq, heads)
    q_spec = pl.BlockSpec((BQ, width), lambda i, *_: (i * parts + half, 0))
    do_spec = pl.BlockSpec((BQ, width), lambda i, *_: (i, 0))
    tab_spec = pl.BlockSpec((BQ, HEAD_DIM), lambda i, *_: (i * parts + half, 0))
    row_spec = pl.BlockSpec((1, 1, heads * BQ), lambda i, *_: (i * parts + half, 0, 0))
    ds_spec = pl.BlockSpec((1, 1, BQ), lambda i, *_: (i * parts + half, 0, 0))
    in_specs = [q_spec, k_spec, v_spec, q_spec, do_spec, row_spec, tab_spec, tab_spec, full_spec, full_spec, ds_spec]
    operands = [lo, full, qkv, qkv, qkv, o, d_o, lse, cos_t, sin_t, cos_t, sin_t, doc_start.reshape(seq // BQ, 1, BQ)]
    aliases = {}
    if half:
        aliases = {len(operands): 0}
        in_specs += [pl.BlockSpec(memory_space=pl.ANY), full_spec, full_spec]
        operands += list(carry)
    dq_shape = jax.ShapeDtypeStruct((seq, width), BF16)
    sum_shape = jax.ShapeDtypeStruct((seq, HEAD_DIM), F32)
    scratch = [pltpu.VMEM((seq, HEAD_DIM), BF16), pltpu.VMEM((heads * BQ, HEAD_DIM), F32)]
    if half == parts - 1:
        out_shape = (dq_shape, jax.ShapeDtypeStruct((seq, 2 * HEAD_DIM), BF16))
        out_specs = [q_spec, pl.BlockSpec((seq, 2 * HEAD_DIM), lambda i, *_: (0, 0))]
        scratch += [pltpu.VMEM((seq, HEAD_DIM), F32)] * 2
    else:
        out_shape = (dq_shape, sum_shape, sum_shape)
        out_specs = [q_spec, full_spec, full_spec]
    return pl.pallas_call(
        functools.partial(bwd_kernel, heads, half, parts, n_blk),
        out_shape=out_shape,
        grid_spec=pltpu.PrefetchScalarGridSpec(num_scalar_prefetch=2, grid=(n_blk,), in_specs=in_specs, out_specs=out_specs, scratch_shapes=scratch),
        input_output_aliases=aliases,
        compiler_params=pltpu.CompilerParams(dimension_semantics=("arbitrary",), vmem_limit_bytes=VMEM_LIMIT),
        cost_estimate=pl.CostEstimate(flops=10 * heads * seq * seq // 2 * HEAD_DIM // parts, bytes_accessed=24 * 2 ** 20 // parts, transcendentals=heads * seq * seq // 2 // parts),
    )(*operands)


def norm_forward(x_f32, norm_gain):
    inv_rms = lax.rsqrt(jnp.mean(x_f32 * x_f32, axis=-1, keepdims=True) + NORM_EPS)
    return (x_f32 * inv_rms * norm_gain).astype(BF16)


def dot32(a, b, dims=(((1,), (0,)), ((), ()))):
    return lax.dot_general(a, b, dims, preferred_element_type=F32)


def sum_over_tp(value, tp_size):
    step = 1
    while step < tp_size:
        value = value + lax.ppermute(value, 'tp', [(d, d ^ step) for d in range(tp_size)])
        step *= 2
    return value


def grad_mm_kernel(width, owner_ref, *refs):
    g_refs, w_refs, (wk_ref, wv_ref, *out_refs, x_s, w_s) = refs[:4], refs[4:8], refs[8:]
    span = width + 2 * HEAD_DIM

    @pl.when(pl.program_id(0) == 0)
    def _():
        for p, g_ref in enumerate(g_refs):
            x_s[:, p * span:(p + 1) * span] = g_ref[0]

    for p, w_ref in enumerate(w_refs):
        head = pl.ds(pl.multiple_of(owner_ref[p] * HEAD_DIM, HEAD_DIM), HEAD_DIM)
        w_s[:, p * span:p * span + width] = w_ref[...]
        w_s[:, p * span + width:p * span + width + HEAD_DIM] = wk_ref[:, head]
        w_s[:, p * span + width + HEAD_DIM:(p + 1) * span] = wv_ref[:, head]
    out = lax.dot_general(x_s[...], w_s[...], NT, preferred_element_type=F32)
    rows = out_refs[0].shape[0]
    for r, out_ref in enumerate(out_refs):
        out_ref[...] = out[r * rows:(r + 1) * rows].astype(out_ref.dtype)


def grad_mm(owners, pieces, half, weights, wk_all, wv_all, dtype, parts=1):
    _, rows, span = pieces[0].shape
    d_model, width = weights[0].shape
    bn = 512
    g_spec = pl.BlockSpec((1, rows, span), lambda j, *_: (half, 0, 0))
    w_spec = pl.BlockSpec((bn, width), lambda j, *_: (j, 0))
    kv_spec = pl.BlockSpec((bn, wk_all.shape[1]), lambda j, *_: (j, 0))
    return pl.pallas_call(
        functools.partial(grad_mm_kernel, width),
        out_shape=[jax.ShapeDtypeStruct((rows // parts, d_model), dtype)] * parts,
        grid_spec=pltpu.PrefetchScalarGridSpec(
            num_scalar_prefetch=1, grid=(d_model // bn,),
            in_specs=[g_spec] * 4 + [w_spec] * 4 + [kv_spec] * 2,
            out_specs=[pl.BlockSpec((rows // parts, bn), lambda j, *_: (0, j))] * parts,
            scratch_shapes=[pltpu.VMEM((rows, 4 * span), BF16), pltpu.VMEM((bn, 4 * span), BF16)]),
        compiler_params=pltpu.CompilerParams(dimension_semantics=("arbitrary",), vmem_limit_bytes=VMEM_LIMIT),
        cost_estimate=pl.CostEstimate(flops=2 * rows * 4 * span * d_model, bytes_accessed=2 * (4 * span + 2 * rows) * d_model, transcendentals=0),
        name="grad_mm",
    )(owners, *pieces, *weights, wk_all, wv_all)


def mix_mm_kernel(width, *refs):
    o_refs, w_refs, (*add_refs, out_ref, x_s, w_s) = refs[:4], refs[4:8], refs[8:]

    @pl.when(pl.program_id(0) == 0)
    def _():
        for p, o_ref in enumerate(o_refs):
            x_s[:, p * width:(p + 1) * width] = o_ref[0]

    for p, w_ref in enumerate(w_refs):
        w_s[p * width:(p + 1) * width, :] = w_ref[...]
    out = jnp.dot(x_s[...], w_s[...], preferred_element_type=F32)
    for add_ref in reversed(add_refs):
        out = out + add_ref[...].astype(F32)
    out_ref[...] = out.astype(out_ref.dtype)


def mix_mm(pieces, half, weights, dtype, added=()):
    _, rows, width = pieces[0].shape
    d_model = weights[0].shape[1]
    bn = 512
    o_spec = pl.BlockSpec((1, rows, width), lambda j: (half, 0, 0))
    w_spec = pl.BlockSpec((width, bn), lambda j: (0, j))
    return pl.pallas_call(
        functools.partial(mix_mm_kernel, width),
        out_shape=jax.ShapeDtypeStruct((rows, d_model), dtype),
        grid=(d_model // bn,),
        in_specs=[o_spec] * 4 + [w_spec] * 4 + [pl.BlockSpec((rows, bn), lambda j: (0, j))] * len(added),
        out_specs=pl.BlockSpec((rows, bn), lambda j: (0, j)),
        scratch_shapes=[pltpu.VMEM((rows, 4 * width), BF16), pltpu.VMEM((4 * width, bn), BF16)],
        compiler_params=pltpu.CompilerParams(dimension_semantics=("arbitrary",), vmem_limit_bytes=VMEM_LIMIT),
        cost_estimate=pl.CostEstimate(flops=2 * rows * 4 * width * d_model, bytes_accessed=2 * (4 * width + 2 * rows) * d_model, transcendentals=0),
        name="mix_mm",
    )(*pieces, *weights, *added)


def finish_kernel(part, own_ref, got_ref, x_ref, dy_ref, gain_ref, *refs):
    dx_ref, dg_ref = refs[-2:]
    x = x_ref[...].astype(F32)
    inv_rms = lax.rsqrt(jnp.mean(x * x, axis=-1, keepdims=True) + NORM_EPS)
    x_hat = x * inv_rms
    d_hidden = (own_ref[...] + got_ref[...].astype(F32)).astype(BF16).astype(F32)

    @pl.when(pl.program_id(0) == 0)
    def _():
        dg_ref[...] = refs[1][...] if part else jnp.zeros_like(dg_ref)

    dg_ref[...] += jnp.sum(d_hidden * x_hat, axis=0, keepdims=True)
    scaled = d_hidden * gain_ref[...]
    d_input = inv_rms * (scaled - x_hat * jnp.mean(scaled * x_hat, axis=-1, keepdims=True))
    dx_ref[...] = (dy_ref[...].astype(F32) + d_input).astype(BF16)


def finish(part, parts, carry, dh_own, dh_got, x_blk, dy_blk, norm_gain):
    rows, d_model = x_blk.shape
    blk_rows = 64
    steps = rows // parts // blk_rows
    blk = pl.BlockSpec((blk_rows, d_model), lambda i: (i + part * steps, 0))
    got = pl.BlockSpec((blk_rows, d_model), lambda i: (i, 0))
    one = pl.BlockSpec((1, d_model), lambda i: (0, 0))
    operands = [dh_own, dh_got, x_blk, dy_blk, norm_gain[None, :]]
    in_specs = [blk, got, blk, blk, one]
    aliases = {}
    if part:
        aliases = {5: 0}
        operands += list(carry)
        in_specs += [pl.BlockSpec(memory_space=pl.ANY), one]
    return pl.pallas_call(
        functools.partial(finish_kernel, part),
        out_shape=(jax.ShapeDtypeStruct((rows, d_model), BF16), jax.ShapeDtypeStruct((1, d_model), F32)),
        grid=(steps,),
        in_specs=in_specs,
        out_specs=[blk, one],
        input_output_aliases=aliases,
        compiler_params=pltpu.CompilerParams(dimension_semantics=("arbitrary",), vmem_limit_bytes=VMEM_LIMIT),
        cost_estimate=pl.CostEstimate(flops=20 * rows * d_model // parts, bytes_accessed=12 * rows * d_model // parts, transcendentals=0),
    )(*operands)


def swap(value, bit, tp_size):
    return lax.ppermute(value, 'tp', [(d, d ^ bit) for d in range(tp_size)])


def pack_kernel(n_in, owner_ref, *refs):
    ins, outs = refs[:4 * n_in], refs[4 * n_in:]
    for p, out_ref in enumerate(outs):
        at = 0
        for ref in ins[p * n_in:(p + 1) * n_in]:
            out_ref[0, :, at:at + ref.shape[2]] = ref[0]
            at += ref.shape[2]


def group_rows(blocks, me, pair_bit, mate_bit, tp_size, gate=None):
    bits = (0, 1, pair_bit, pair_bit | 1)
    owners = jnp.stack([me ^ bit ^ mate for bit in bits for mate in (0, mate_bit)])
    rows = blocks[0].shape[1]
    span = sum(b.shape[2] for b in blocks)
    in_specs = [pl.BlockSpec((1, rows, b.shape[2]), functools.partial(lambda p, h, owner: (owner[2 * p + h], 0, 0), p)) for p in range(4) for b in blocks]
    sent = pl.pallas_call(
        functools.partial(pack_kernel, len(blocks)),
        out_shape=[jax.ShapeDtypeStruct((2, rows, span), BF16)] * 4,
        grid_spec=pltpu.PrefetchScalarGridSpec(num_scalar_prefetch=1, grid=(2,), in_specs=in_specs,
                                               out_specs=[pl.BlockSpec((1, rows, span), lambda h, owner: (h, 0, 0))] * 4),
        compiler_params=pltpu.CompilerParams(dimension_semantics=("arbitrary",), vmem_limit_bytes=VMEM_LIMIT),
        cost_estimate=pl.CostEstimate(flops=0, bytes_accessed=32 * rows * span, transcendentals=0),
        name="pack_rows",
    )(owners, *(list(blocks) * 4))
    if gate is not None:
        sent = lax.optimization_barrier((*sent, gate))[:4]
    pieces = [sent[0]]
    for bit, rows_sent in zip(bits[1:], sent[1:]):
        pieces.append(swap(rows_sent, bit, tp_size))
    return pieces


def solution(mesh):
    tp_size = mesh.shape['tp']
    x_bit, y_bit = 2, 4

    def layer(x_blk, dy_blk, positions, norm_gain, wq_loc, wk_all, wv_all, wo_loc):
        heads = wq_loc.shape[1] // HEAD_DIM
        width = heads * HEAD_DIM
        rows, _ = x_blk.shape
        me = lax.axis_index('tp')

        def head_of(weights, owner):
            return lax.dynamic_slice_in_dim(weights, owner * HEAD_DIM, HEAD_DIM, axis=1)

        wqkv = jnp.concatenate([wq_loc, head_of(wk_all, me), head_of(wv_all, me)], axis=1)

        x_f32 = x_blk.astype(F32)
        hidden = norm_forward(x_f32, norm_gain)
        h_full = lax.all_gather(hidden, 'tp', axis=0, tiled=True)
        seq = h_full.shape[0]
        parts = rows // BQ
        dy_late, _ = lax.optimization_barrier((dy_blk, hidden))
        dy_in = [dy_late[p * BQ:(p + 1) * BQ] for p in range(parts)]
        dy_full = [lax.all_gather(dy_in[0], 'tp', axis=0, tiled=True)]

        cos_t, sin_t = rope_tables(positions)
        doc_start = lax.iota(jnp.int32, seq) - positions
        lo, lo_bwd = doc_start[::BQ] // BK, doc_start[::BQ] // BK_BWD
        full, full_bwd = (doc_start[BQ - 1::BQ] + BK - 1) // BK, (doc_start[BQ - 1::BQ] + BK_BWD - 1) // BK_BWD

        h_full, cos_t, sin_t, lo, full, doc_start, wqkv = lax.optimization_barrier((h_full, cos_t, sin_t, lo, full, doc_start, wqkv))
        qkv = dot32(h_full, wqkv).astype(BF16)
        *dy_rest, qkv = lax.optimization_barrier((*dy_in[1:], qkv))
        dy_full += [lax.all_gather(dy_part, 'tp', axis=0, tiled=True) for dy_part in dy_rest]
        o, lse = attend_forward(lo, full, qkv, cos_t, sin_t, doc_start, heads)
        dy_full[0], o = lax.optimization_barrier((dy_full[0], o))
        o_blocks = o.reshape(tp_size, parts, BQ, width)
        carry = None
        for p in range(parts - 1):
            d_o = dot32(dy_full[p], wo_loc, NT).astype(BF16)
            carry = attend_backward(p, parts, carry, lo_bwd, full_bwd, qkv, o, d_o, lse, cos_t, sin_t, doc_start, heads)
        o_first, _ = lax.optimization_barrier((o_blocks[:, 0], carry[0]))
        d_wo = dot32(o_first.reshape(-1, width), dy_full[0], TN)
        dy_full[-1], d_wo = lax.optimization_barrier((dy_full[-1], d_wo))
        dy_full[-1], wo_own, wq_own = lax.optimization_barrier((dy_full[-1], wo_loc, wq_loc))
        wq_near = swap(wq_own, y_bit, tp_size)
        wo_near = swap(wo_own, x_bit, tp_size)
        o_pieces = group_rows([o.reshape(tp_size, rows, width)], me, x_bit, y_bit, tp_size, dy_full[-1])

        d_o = dot32(dy_full[-1], wo_loc, NT).astype(BF16)
        d_q, d_kv = attend_backward(parts - 1, parts, carry, lo_bwd, full_bwd, qkv, o, d_o, lse, cos_t, sin_t, doc_start, heads)
        dq_pieces = group_rows([d_q.reshape(tp_size, rows, width), d_kv.reshape(tp_size, rows, 2 * HEAD_DIM)], me, y_bit, x_bit, tp_size)
        d_wq = dot32(h_full, d_q, TN).astype(BF16)
        d_wkv = dot32(h_full, d_kv, TN)
        wq_near, wq_own, wo_near, wo_own, d_wq = lax.optimization_barrier((wq_near, wq_own, wo_near, wo_own, d_wq))
        wo_side = swap(wo_own, 1, tp_size)
        wo_group = [wo_own, wo_side, wo_near, swap(wo_near, 1, tp_size)]
        wq_side = swap(wq_own, 1, tp_size)
        wq_group = [wq_own, wq_side, wq_near, swap(wq_near, 1, tp_size)]
        mix_mate = mix_mm(o_pieces, 1, wo_group, BF16)
        dq_pieces, mix_mate, d_wq, d_wkv = lax.optimization_barrier((dq_pieces, mix_mate, d_wq, d_wkv))
        mix_got = swap(mix_mate, y_bit, tp_size)
        owners = jnp.stack([me ^ bit for bit in (0, 1, y_bit, y_bit | 1)])
        halves = 2
        dh_mate = list(grad_mm(owners, dq_pieces, 1, wq_group, wk_all, wv_all, BF16, halves))
        o_blocks, d_wkv, dh_mate[0] = lax.optimization_barrier((o_blocks, d_wkv, dh_mate[0]))
        for p in range(1, parts):
            d_wo = d_wo + dot32(o_blocks[:, p].reshape(-1, width), dy_full[p], TN)
        d_wo = d_wo.astype(BF16)
        dh_got = []
        for p in range(halves):
            dh_got.append(swap(dh_mate[p], x_bit, tp_size))
        dh_own, = grad_mm(owners, dq_pieces, 0, wq_group, wk_all, wv_all, F32)
        mix_own = mix_mm(o_pieces, 0, wo_group, F32, (x_blk,))
        d_wk, d_wv = d_wkv[:, :HEAD_DIM], d_wkv[:, HEAD_DIM:]
        dh_own, dh_got[0], mix_own, d_wo, d_wk, d_wv = lax.optimization_barrier((dh_own, dh_got[0], mix_own, d_wo, d_wk, d_wv))
        done = finish(0, halves, None, dh_own, dh_got[0], x_blk, dy_blk, norm_gain)
        result = (mix_own + mix_got.astype(F32)).astype(BF16)
        result, dh_got[1] = lax.optimization_barrier((result, dh_got[1]))
        done = finish(1, halves, done, dh_own, dh_got[1], x_blk, dy_blk, norm_gain)
        grad_x, d_gain = done[0], sum_over_tp(done[1][0], tp_size)
        return result, grad_x, d_wq, d_wk, d_wv, d_wo, d_gain

    specs_in = (P(('dp', 'tp'), None), P(('dp', 'tp'), None), P('dp'), P(), P(None, 'tp'), P(), P(), P('tp', None))
    specs_out = (P(('dp', 'tp'), None), P(('dp', 'tp'), None), P('dp', 'tp'), P('dp', 'tp'), P('dp', 'tp'), P(('dp', 'tp'), None), P('dp'))
    return jax.shard_map(layer, mesh=mesh, in_specs=specs_in, out_specs=specs_out, check_vma=False)
```
